32 devices in a mesh: gx: 4 (over y, x), gy: 8 (over z, core).
Axes of the slice: x: 2, y: 2, z: 4, core: 2. Of those that a mesh axis runs over, the one named last changes fastest.
Arguments:
- positions: float32 [3, 524288], P(None, ('gx', 'gy')), may hold values from -6 to 6
- normals: float32 [3, 524288], P(None, ('gx', 'gy')), may hold values from -6 to 6
- areas: float32 [524288], P(('gx', 'gy')), may hold values from 0.5 to 2
- pair_first: int32 [4096], P(('gx', 'gy')), may hold values from 0 to 2047, as said below
- pair_second: int32 [4096], P(('gx', 'gy')), may hold values from 0 to 2047, as said below
- pair_count: int32 [32], P(('gx', 'gy')), may hold values from 32 to 128, as said below
Outputs:
- gradient: float32 [3, 524288], P(None, ('gx', 'gy'))
The draws below stay inside these ranges and needn't reach their ends.
Inputs may be any that keep to these rules, and one draw needn't show every extreme that they name: `pair_first`: slot s holds a first cluster owned by device s // 128, that is in s // 128 * 64 to (s // 128 + 1) * 64 - 1. `pair_second`: the second cluster of slot s lies on a device at most 2 away from s // 128: its index // 64 differs from s // 128 by at most 2. Dead slots hold such pairs too. `pair_count`: some device has all 128 slots live in every draw.
All inputs are finite; a program needn't handle non-finite values.
Results may differ from the reference program's by a relative error of at most 0.0001.
Values sent between devices are 32-bit elements; how exact they have to be, the bound alone decides.
No kernel may reach another device: no remote copies, remote signals or barrier semaphores. Data moves between devices by JAX's collectives and lax.ppermute only.
A program may use at most 64 MiB of HBM per device.

```python
import math
import jax
import jax.numpy as jnp
from jax import lax

C = 256
CL_DEV = 64
PAIR_CAP = 128
REACH = 2
BLOCK = 4
NC = 2048
FACES = 524288


def draw_pair_first(key, part):
    devices = NC // CL_DEV
    total = devices * PAIR_CAP
    owner = jnp.arange(total, dtype=jnp.int32) // PAIR_CAP
    local = jax.random.randint(jax.random.fold_in(key, 11), (total,), 0, CL_DEV, dtype=jnp.int32)
    return (owner * CL_DEV + local).astype(jnp.int32)


def draw_pair_second(key, part):
    devices = NC // CL_DEV
    total = devices * PAIR_CAP
    owner = jnp.arange(total, dtype=jnp.int32) // PAIR_CAP
    offset = jax.random.randint(jax.random.fold_in(key, 23), (total,), -REACH, REACH + 1, dtype=jnp.int32)
    target = jnp.clip(owner + offset, 0, devices - 1)
    local = jax.random.randint(jax.random.fold_in(key, 37), (total,), 0, CL_DEV, dtype=jnp.int32)
    return (target * CL_DEV + local).astype(jnp.int32)


def draw_pair_count(key, part):
    devices = NC // CL_DEV
    level = jax.random.randint(jax.random.fold_in(key, 41), (devices,), 0, 8, dtype=jnp.int32)
    fullest = jax.random.randint(jax.random.fold_in(key, 53), (), 0, devices, dtype=jnp.int32)
    level = jnp.where(jnp.arange(devices, dtype=jnp.int32) == fullest, 7, level)
    lowest = PAIR_CAP // 4
    return (lowest + (PAIR_CAP - lowest) * level * level // 49).astype(jnp.int32)


def block_levels(key, extent, split, low, high):
    level = 1.0
    for axis_at, shards_of in split:
        draws = jax.random.uniform(jax.random.fold_in(jax.random.fold_in(key, 6), axis_at), (shards_of,), jnp.float32, low / len(split), high / len(split))
        level = level * jnp.repeat(jnp.exp(draws), extent[axis_at] // shards_of).reshape((-1,) + (1,) * (len(extent) - 1 - axis_at))
    return level


def gaussian(rng, shape, spread, bound, cuts=(), held_as=jnp.bfloat16):
    array = jax.random.normal(rng, shape, jnp.float32) * spread
    if len(cuts) > 0:
        array = block_levels(rng, shape, cuts, -0.22, 0.18) * array
    return jnp.clip(array, min=-bound, max=bound).astype(held_as)


def setup_inputs(seed: int = 0) -> dict:
    key_of = jax.random.split(jax.random.key(seed), 7)
    positions = gaussian(key_of[0], (3, FACES), 1.0, 6.0, ((1, 32),), jnp.float32)
    normals = gaussian(key_of[1], (3, FACES), 1.0, 6.0, ((1, 32),), jnp.float32)
    areas = jnp.clip(jnp.exp(math.log(2.0) - 1.3862944 * jax.random.uniform(key_of[2], (FACES,), jnp.float32) ** block_levels(key_of[2], (FACES,), ((0, 32),), -0.2, 0.2)), 0.5, 2.0)
    pair_first = draw_pair_first(jax.random.fold_in(key_of[6], 71), 0)
    pair_second = draw_pair_second(jax.random.fold_in(key_of[6], 71), 0)
    pair_count = draw_pair_count(jax.random.fold_in(key_of[6], 71), 0)
    return {"positions": positions, "normals": normals, "areas": areas, "pair_first": pair_first, "pair_second": pair_second, "pair_count": pair_count}


def tile_terms(pos_f, nor_f, area_f, pos_g, nor_g, area_g):
    delta = [pos_f[:, k, :, None] - pos_g[:, k, None, :] for k in range(3)]
    radius = delta[0] * delta[0] + delta[1] * delta[1] + delta[2] * delta[2] + 1.0
    inverse = 1.0 / radius
    weight = area_f[:, :, None] * area_g[:, None, :] * inverse * inverse * inverse
    along_f = nor_f[:, 0, :, None] * delta[0] + nor_f[:, 1, :, None] * delta[1] + nor_f[:, 2, :, None] * delta[2]
    along_g = nor_g[:, 0, None, :] * delta[0] + nor_g[:, 1, None, :] * delta[1] + nor_g[:, 2, None, :] * delta[2]
    linear_f = 2.0 * weight * along_f
    linear_g = 2.0 * weight * along_g
    radial = -6.0 * weight * inverse * (along_f * along_f + along_g * along_g)
    grad_first = []
    grad_second = []
    for k in range(3):
        comp = linear_f * nor_f[:, k, :, None] + linear_g * nor_g[:, k, None, :] + radial * delta[k]
        grad_first.append(jnp.sum(comp, axis=2))
        grad_second.append(-jnp.sum(comp, axis=1))
    return jnp.stack(grad_first, axis=1), jnp.stack(grad_second, axis=1)


def reference(positions, normals, areas, pair_first, pair_second, pair_count):
    pos = positions.reshape(3, NC, C).transpose(1, 0, 2)
    nor = normals.reshape(3, NC, C).transpose(1, 0, 2)
    area = areas.reshape(NC, C)
    total = pair_first.shape[0]
    slots = jnp.arange(total, dtype=jnp.int32)
    owners = slots // PAIR_CAP
    live = ((slots % PAIR_CAP) < pair_count[owners]).astype(jnp.float32)
    firsts = pair_first.reshape(total // BLOCK, BLOCK)
    seconds = pair_second.reshape(total // BLOCK, BLOCK)
    lives = live.reshape(total // BLOCK, BLOCK)

    def step(grad, inputs):
        first, second, alive = inputs
        grad_first, grad_second = tile_terms(pos[first], nor[first], area[first], pos[second], nor[second], area[second])
        grad = grad.at[first].add(grad_first * alive[:, None, None])
        grad = grad.at[second].add(grad_second * alive[:, None, None])
        return grad, None

    start = jnp.zeros((NC, 3, C), jnp.float32)
    grad, unused = lax.scan(step, start, (firsts, seconds, lives))
    return grad.transpose(1, 0, 2).reshape(3, NC * C)
```

```python
import jax
import jax.numpy as jnp
from jax import lax
from jax.experimental import pallas as pl
from jax.experimental.pallas import tpu as pltpu
from jax.sharding import PartitionSpec as P

C = 256
AXES = ("gx", "gy")
UNROLL = 4
ROWS = 32
F32 = jnp.float32
BF16 = jnp.bfloat16
NN = ((1,), (0,))
NT = ((1,), (1,))
TN = ((0,), (0,))


def dot(a, b, dims):
    return lax.dot_general(a, b, (dims, ((), ())), preferred_element_type=F32)


def rounded(x):
    return x.astype(BF16).astype(F32)


def two_tiles(ref, base, pitch, n):
    return jnp.concatenate([ref[pl.ds(base, n), :], ref[pl.ds(base + pitch, n), :]], axis=1)


def features(block, feat_g, g_base, feat_f):
    zero = jnp.zeros((8, 128), F32)
    one = jnp.ones((8, 128), F32)

    def step(j, carry):
        p0, p1, p2, n0, n1, n2, s = [block[pl.ds(j * 64 + k, 8, stride=8), :] for k in range(7)]
        pp = (p0 * p0 + p1 * p1 + p2 * p2 + 0.5) * s
        dot_np = n0 * p0 + n1 * p1 + n2 * p2
        q0, q1, q2 = p0 * s, p1 * s, p2 * s
        g_rows = (q0, q1, q2, pp, s, zero, zero, zero, p0, p1, p2, n0, n1, n2, dot_np, one)
        for r, v in enumerate(g_rows):
            feat_g[pl.ds(g_base + j * 128 + r, 8, stride=16), :] = v
        if feat_f is not None:
            f_rows = (-2.0 * q0, -2.0 * q1, -2.0 * q2, s, pp, zero, zero, zero)
            f_rows += (-n0, -n1, -n2, zero, zero, zero, zero, dot_np)
            f_rows += (zero, zero, zero, p0, p1, p2, -one, zero)
            for r, v in enumerate(f_rows):
                feat_f[pl.ds(j * 192 + r, 8, stride=24), :] = v
        return carry

    lax.fori_loop(0, block.shape[0] // 64, step, 0)


def pair_loop(first, second, start, stop, feat_f, feat_g, acc, dummy, scratch):
    forms, terms, weights, row_part, col_part = scratch

    def clusters(t):
        live = jnp.logical_and(t >= start, t < stop)
        safe = jnp.clip(t, 0, first.shape[0] - 1)
        a = first[safe]
        b = second[safe]
        return a, b, jnp.where(live, a, dummy), jnp.where(live, b, dummy)

    def stage(t, par):
        form_w, form_r = forms[par], forms[1 - par]
        term_w, term_r = terms[1 - par], terms[par]
        state = {}

        def prepare():
            a, b, _, _ = clusters(t)
            f = two_tiles(feat_f, pl.multiple_of(a * 48, 8), 24, 24)
            g = two_tiles(feat_g, pl.multiple_of(b * 32, 8), 16, 16)
            f1 = rounded(f)
            rest = f - f1
            f2 = rounded(rest)
            f3 = rest - f2
            g1 = rounded(g)
            rest = g - g1
            g2 = rounded(rest)
            g3 = rest - g2
            state["f"] = (f1, f2)
            state["g"] = (g1, g2)
            state["left"] = []
            for k in range(3):
                at = slice(8 * k, 8 * k + 8)
                state["left"].append(
                    jnp.concatenate([f1[at], f2[at], f3[at], f1[at], f2[at], f1[at]], axis=0)
                )
            state["right"] = []
            for k in range(2):
                at = slice(8 * k, 8 * k + 8)
                state["right"].append(
                    jnp.concatenate([g1[at], g1[at], g1[at], g2[at], g2[at], g3[at]], axis=0)
                )

        def form(k):
            def run():
                form_w[k] = dot(state["left"][k], state["right"][min(k, 1)], TN)

            return run

        def keep_weights():
            f1, f2 = state["f"]
            g1, g2 = state["g"]
            for k, (x, y) in enumerate(((f1, f2), (g1, g2))):
                for h in range(2):
                    at = slice(8 * h, 8 * h + 8)
                    rows = slice(32 * k + 16 * h, 32 * k + 16 * h + 16)
                    weights[par][rows] = jnp.concatenate([x[at], y[at]], axis=0).astype(BF16)

        col_sum = []

        def term(c):
            def run():
                rows = pl.ds(c * ROWS, ROWS)
                r2 = form_r[0, rows, :]
                sf = form_r[1, rows, :]
                sg = form_r[2, rows, :]
                inv = 1.0 / r2
                w = inv * inv * inv
                a = w * sf
                b = w * sg
                q = inv * (sf * a + sg * b)
                for m, v in enumerate((a, b, q)):
                    high = v.astype(BF16)
                    term_w[2 * m, rows, :] = high
                    term_w[2 * m + 1, rows, :] = (v - high.astype(F32)).astype(BF16)
                row_part[1 - par][rows, :] = a[:, :128] + a[:, 128:]
                part = b[0:8]
                for i in range(1, ROWS // 8):
                    part = part + b[8 * i : 8 * i + 8]
                col_sum.append(part)

            return run

        sums = {}

        def reduce(name, row, m, dims):
            def run():
                o = dot(weights[par][row : row + 16], term_r[m], dims)
                sums[name] = sums[name] + o if name in sums else o

            return run

        def plain_sums():
            turned = jnp.transpose(row_part[par][...])
            total = turned[0:8]
            for i in range(1, 16):
                total = total + turned[8 * i : 8 * i + 8]
            sums["a"] = jnp.sum(total, axis=0, keepdims=True)
            sums["b"] = jnp.sum(col_part[par][...], axis=0, keepdims=True)

        def finish():
            a, b, a_to, b_to = clusters(t - 2)

            def joined(x):
                return x[0:8] + x[8:16]

            def wide(x):
                return jnp.broadcast_to(x, (8, 256))

            col_q, col_a = joined(sums["col_q"]), joined(sums["col_a"])
            row_q, row_b = joined(sums["row_q"]), joined(sums["row_b"])
            fr = two_tiles(feat_f, pl.multiple_of(a * 48, 8), 24, 8)
            fs = two_tiles(feat_f, pl.multiple_of(a * 48 + 8, 8), 24, 8)
            gp = two_tiles(feat_g, pl.multiple_of(b * 32, 8), 16, 8)
            gq = two_tiles(feat_g, pl.multiple_of(b * 32 + 8, 8), 16, 8)
            grad_f = 3.0 * fr * wide(row_q[4:5]) + 6.0 * wide(fr[3:4]) * row_q
            grad_f = grad_f - 2.0 * fs * wide(sums["a"]) + 2.0 * pltpu.roll(row_b, 5, 0)
            grad_g = 2.0 * col_a - 2.0 * wide(sums["b"]) * pltpu.roll(gq, 5, 0)
            grad_g = grad_g - 3.0 * wide(gp[4:5]) * col_q - 6.0 * gp * wide(col_q[3:4])
            for c, g in ((a_to, grad_f), (b_to, grad_g)):
                at = pl.multiple_of(c * 16, 8)
                acc[pl.ds(at, 8), :] += g[:, :128]
                acc[pl.ds(at + 8, 8), :] += g[:, 128:]

        others = [
            prepare,
            reduce("col_a", 16, 0, NN),
            reduce("col_a", 16, 1, NN),
            form(0),
            form(1),
            form(2),
            reduce("col_q", 0, 4, NN),
            reduce("col_q", 0, 5, NN),
            reduce("row_q", 32, 4, NT),
            reduce("row_q", 32, 5, NT),
            reduce("row_b", 48, 2, NT),
            reduce("row_b", 48, 3, NT),
            plain_sums,
            finish,
            keep_weights,
        ]
        chunks = 256 // ROWS
        each = -(-len(others) // chunks)
        for c in range(chunks):
            for other in others[each * c : each * c + each]:
                other()
            term(c)()
        total = col_sum[0]
        for part in col_sum[1:]:
            total = total + part
        col_part[1 - par][...] = total

    def body(i, carry):
        for u in range(UNROLL):
            stage(start + i * UNROLL + u, u % 2)
        return carry

    trips = jnp.where(stop > start, (stop - start + 2 + UNROLL - 1) // UNROLL, 0)
    lax.fori_loop(0, trips, body, 0)


def kernel(first, second, scalars, b0, b1, b3, b4, own, near, far, feat_f, feat_g, acc, *scratch):
    rows = b0.shape[0]
    acc[...] = jnp.zeros_like(acc)
    blocks = (b0, b1.at[0:rows], b1.at[rows : 2 * rows], b3, b4)
    for k, block in enumerate(blocks):
        features(block, feat_g, k * 2 * rows, feat_f if k == 0 else None)
    pairs = [scratch[2 * k : 2 * k + 2] for k in range(5)]
    dummy = 5 * rows // 16
    pair_loop(first, second, 0, scalars[0], feat_f, feat_g, acc, dummy, pairs)
    tiles = rows // 8
    for k in range(5):
        out, base = ((own, 0), (near, 0), (near, 3 * tiles), (far, 0), (far, 3 * tiles))[k]
        for r in range(3):
            out[pl.ds(base + r * tiles, tiles), :] = acc[pl.ds(k * rows + r, tiles, stride=8), :]


def body(positions, normals, areas, pair_first, pair_second, pair_count):
    faces = areas.shape[0]
    clusters = faces // C
    tiles = faces // 128
    rows = 8 * tiles
    devices = lax.axis_size(AXES)
    me = lax.axis_index(AXES)
    odd = me % 2
    scale = jnp.exp(jnp.log(areas) * (-1.0 / 3.0))
    geometry = jnp.concatenate(
        [positions, normals, scale[None, :], jnp.zeros((1, faces), F32)], axis=0
    )
    geometry = geometry.reshape(8, tiles, 128).transpose(1, 0, 2).reshape(rows, 128)

    def shift(x, by):
        pairs = [(i, i + by) for i in range(devices) if 0 <= i + by < devices]
        return lax.ppermute(x, AXES, pairs)

    def swap(x):
        return lax.ppermute(x, AXES, [(i, i ^ 1) for i in range(devices)])

    minus2 = shift(geometry, 2)
    plus2 = shift(geometry, -2)
    relay = jnp.where(odd == 1, minus2, plus2)
    near_blocks = swap(jnp.concatenate([geometry, relay], axis=0))

    delta = pair_second // clusters - me
    toward = delta * (1 - 2 * odd)
    place = jnp.where(toward == 1, 1, jnp.where(toward == -1, 2, 0))
    place = jnp.where(delta == -2, 3, jnp.where(delta == 2, 4, place))
    first = pair_first - me * clusters
    second = place * clusters + pair_second % clusters

    smem = pl.BlockSpec(memory_space=pltpu.SMEM)
    vmem = pl.BlockSpec(memory_space=pltpu.VMEM)
    part = 3 * tiles
    own, near, far = pl.pallas_call(
        kernel,
        out_shape=[
            jax.ShapeDtypeStruct((part, 128), F32),
            jax.ShapeDtypeStruct((2 * part, 128), F32),
            jax.ShapeDtypeStruct((2 * part, 128), F32),
        ],
        in_specs=[smem] * 3 + [vmem] * 4,
        out_specs=[vmem] * 3,
        scratch_shapes=[
            pltpu.VMEM((3 * rows, 128), F32),
            pltpu.VMEM((10 * rows, 128), F32),
            pltpu.VMEM((5 * rows + 16, 128), F32),
        ]
        + [pltpu.VMEM((3, 256, 256), F32)] * 2
        + [pltpu.VMEM((6, 256, 256), BF16)] * 2
        + [pltpu.VMEM((64, 256), BF16)] * 2
        + [pltpu.VMEM((256, 128), F32)] * 2
        + [pltpu.VMEM((8, 256), F32)] * 2,
        compiler_params=pltpu.CompilerParams(
            vmem_limit_bytes=60 * 2**20,
        ),
        name="pairs",
    )(first, second, pair_count, geometry, near_blocks, minus2, plus2)

    got = swap(near)
    pass_on = got[part:]
    to_minus = far[:part] + jnp.where(odd == 1, pass_on, 0.0)
    to_plus = far[part:] + jnp.where(odd == 0, pass_on, 0.0)
    total = own + got[:part] + shift(to_minus, -2) + shift(to_plus, 2)
    return total.reshape(3, faces)


def solution(mesh):
    in_specs = (
        P(None, AXES),
        P(None, AXES),
        P(AXES),
        P(AXES),
        P(AXES),
        P(AXES),
    )
    return jax.shard_map(
        body, mesh=mesh, in_specs=in_specs, out_specs=P(None, AXES), check_vma=False
    )
```

```python
import functools

import jax
import jax.numpy as jnp
from jax import lax
from jax.experimental import pallas as pl
from jax.experimental.pallas import tpu as pltpu
from jax.sharding import PartitionSpec as P

C = 256
AXES = ("gx", "gy")
UNROLL = 4
ROWS = 32
F32 = jnp.float32
BF16 = jnp.bfloat16
NN = ((1,), (0,))
NT = ((1,), (1,))
TN = ((0,), (0,))


def dot(a, b, dims):
    return lax.dot_general(a, b, (dims, ((), ())), preferred_element_type=F32)


def rounded(x):
    return x.astype(BF16).astype(F32)


def two_tiles(ref, base, pitch, n):
    return jnp.concatenate([ref[pl.ds(base, n), :], ref[pl.ds(base + pitch, n), :]], axis=1)


def features(block, feat_g, g_base, feat_f):
    zero = jnp.zeros((8, 128), F32)
    one = jnp.ones((8, 128), F32)

    def step(j, carry):
        p0, p1, p2, n0, n1, n2, area = [block[pl.ds(j * 56 + k, 8, stride=7), :] for k in range(7)]
        s = jnp.exp(jnp.log(area) * (-1.0 / 3.0))
        pp = (p0 * p0 + p1 * p1 + p2 * p2 + 0.5) * s
        dot_np = n0 * p0 + n1 * p1 + n2 * p2
        q0, q1, q2 = p0 * s, p1 * s, p2 * s
        g_rows = (q0, q1, q2, pp, s, zero, zero, zero, p0, p1, p2, n0, n1, n2, dot_np, one)
        for r, v in enumerate(g_rows):
            feat_g[pl.ds(g_base + j * 128 + r, 8, stride=16), :] = v
        if feat_f is not None:
            f_rows = (-2.0 * q0, -2.0 * q1, -2.0 * q2, s, pp, zero, zero, zero)
            f_rows += (-n0, -n1, -n2, zero, zero, zero, zero, dot_np)
            f_rows += (zero, zero, zero, p0, p1, p2, -one, zero)
            for r, v in enumerate(f_rows):
                feat_f[pl.ds(j * 192 + r, 8, stride=24), :] = v
        return carry

    lax.fori_loop(0, block.shape[0] // 56, step, 0)


def pair_loop(first, second, start, stop, feat_f, feat_g, acc, dummy, scratch):
    forms, terms, weights, row_part, col_part = scratch

    def clusters(t):
        live = jnp.logical_and(t >= start, t < stop)
        safe = jnp.clip(t, start, stop - 1)
        a = first[safe]
        b = second[safe]
        return a, b, jnp.where(live, a, dummy), jnp.where(live, b, dummy)

    def stage(t, par):
        form_w, form_r = forms[par], forms[1 - par]
        term_w, term_r = terms[1 - par], terms[par]
        state = {}

        def prepare():
            a, b, _, _ = clusters(t)
            f = two_tiles(feat_f, pl.multiple_of(a * 48, 8), 24, 24)
            g = two_tiles(feat_g, pl.multiple_of(b * 32, 8), 16, 16)
            f1 = rounded(f)
            rest = f - f1
            f2 = rounded(rest)
            f3 = rest - f2
            g1 = rounded(g)
            rest = g - g1
            g2 = rounded(rest)
            g3 = rest - g2
            state["f"] = (f1, f2)
            state["g"] = (g1, g2)
            state["left"] = []
            for k in range(3):
                at = slice(8 * k, 8 * k + 8)
                state["left"].append(
                    jnp.concatenate([f1[at], f2[at], f3[at], f1[at], f2[at], f1[at]], axis=0)
                )
            state["right"] = []
            for k in range(2):
                at = slice(8 * k, 8 * k + 8)
                state["right"].append(
                    jnp.concatenate([g1[at], g1[at], g1[at], g2[at], g2[at], g3[at]], axis=0)
                )

        def form(k):
            def run():
                form_w[k] = dot(state["left"][k], state["right"][min(k, 1)], TN)

            return run

        def keep_weights():
            f1, f2 = state["f"]
            g1, g2 = state["g"]
            for k, (x, y) in enumerate(((f1, f2), (g1, g2))):
                for h in range(2):
                    at = slice(8 * h, 8 * h + 8)
                    rows = slice(32 * k + 16 * h, 32 * k + 16 * h + 16)
                    weights[par][rows] = jnp.concatenate([x[at], y[at]], axis=0).astype(BF16)

        col_sum = []

        def term(c):
            def run():
                rows = pl.ds(c * ROWS, ROWS)
                r2 = form_r[0, rows, :]
                sf = form_r[1, rows, :]
                sg = form_r[2, rows, :]
                inv = 1.0 / r2
                w = inv * inv * inv
                a = w * sf
                b = w * sg
                q = inv * (sf * a + sg * b)
                for m, v in enumerate((a, b, q)):
                    high = v.astype(BF16)
                    term_w[2 * m, rows, :] = high
                    term_w[2 * m + 1, rows, :] = (v - high.astype(F32)).astype(BF16)
                row_part[1 - par][rows, :] = a[:, :128] + a[:, 128:]
                part = b[0:8]
                for i in range(1, ROWS // 8):
                    part = part + b[8 * i : 8 * i + 8]
                col_sum.append(part)

            return run

        sums = {}

        def reduce(name, row, m, dims):
            def run():
                o = dot(weights[par][row : row + 16], term_r[m], dims)
                sums[name] = sums[name] + o if name in sums else o

            return run

        def plain_sums():
            turned = jnp.transpose(row_part[par][...])
            total = turned[0:8]
            for i in range(1, 16):
                total = total + turned[8 * i : 8 * i + 8]
            sums["a"] = jnp.sum(total, axis=0, keepdims=True)
            sums["b"] = jnp.sum(col_part[par][...], axis=0, keepdims=True)

        def finish():
            a, b, a_to, b_to = clusters(t - 2)

            def joined(x):
                return x[0:8] + x[8:16]

            def wide(x):
                return jnp.broadcast_to(x, (8, 256))

            col_q, col_a = joined(sums["col_q"]), joined(sums["col_a"])
            row_q, row_b = joined(sums["row_q"]), joined(sums["row_b"])
            fr = two_tiles(feat_f, pl.multiple_of(a * 48, 8), 24, 8)
            fs = two_tiles(feat_f, pl.multiple_of(a * 48 + 8, 8), 24, 8)
            gp = two_tiles(feat_g, pl.multiple_of(b * 32, 8), 16, 8)
            gq = two_tiles(feat_g, pl.multiple_of(b * 32 + 8, 8), 16, 8)
            grad_f = 3.0 * fr * wide(row_q[4:5]) + 6.0 * wide(fr[3:4]) * row_q
            grad_f = grad_f - 2.0 * fs * wide(sums["a"]) + 2.0 * pltpu.roll(row_b, 5, 0)
            grad_g = 2.0 * col_a - 2.0 * wide(sums["b"]) * pltpu.roll(gq, 5, 0)
            grad_g = grad_g - 3.0 * wide(gp[4:5]) * col_q - 6.0 * gp * wide(col_q[3:4])
            for c, g in ((a_to, grad_f), (b_to, grad_g)):
                at = pl.multiple_of(c * 16, 8)
                acc[pl.ds(at, 8), :] += g[:, :128]
                acc[pl.ds(at + 8, 8), :] += g[:, 128:]

        others = [
            prepare,
            reduce("col_a", 16, 0, NN),
            reduce("col_a", 16, 1, NN),
            form(0),
            form(1),
            form(2),
            reduce("col_q", 0, 4, NN),
            reduce("col_q", 0, 5, NN),
            reduce("row_q", 32, 4, NT),
            reduce("row_q", 32, 5, NT),
            reduce("row_b", 48, 2, NT),
            reduce("row_b", 48, 3, NT),
            plain_sums,
            finish,
            keep_weights,
        ]
        chunks = 256 // ROWS
        each = -(-len(others) // chunks)
        for c in range(chunks):
            for other in others[each * c : each * c + each]:
                other()
            term(c)()
        total = col_sum[0]
        for part in col_sum[1:]:
            total = total + part
        col_part[1 - par][...] = total

    def body(i, carry):
        for u in range(UNROLL):
            stage(start + i * UNROLL + u, u % 2)
        return carry

    trips = jnp.where(stop > start, (stop - start + 2 + UNROLL - 1) // UNROLL, 0)
    lax.fori_loop(0, trips, body, 0)


def kernel(classes, first, second, kind, count, own_block, *refs):
    n = len(classes)
    blocks = refs[: n - 1]
    outs = refs[n - 1 : 2 * n - 1]
    feat_f, feat_g, acc, list_a, list_b = refs[2 * n - 1 : 2 * n + 4]
    scratch = refs[2 * n + 4 :]
    tiles = own_block.shape[0] // 7
    rows = 8 * tiles
    slots = first.shape[0]

    def pick(s, found):
        list_a[found] = first[s]
        place = n
        for k, c in enumerate(classes):
            place = jnp.where(kind[s] == c, k, place)
        list_b[found] = second[s] + place * (rows // 16)
        take = jnp.logical_and(place < n, s < count[0])
        return found + take.astype(jnp.int32)

    stop = lax.fori_loop(0, slots, pick, 0, unroll=8)
    acc[...] = jnp.zeros_like(acc)
    features(own_block, feat_g, 0, feat_f)
    for k, block in enumerate(blocks):
        features(block, feat_g, (k + 1) * 2 * rows, None)
    pairs = [scratch[2 * k : 2 * k + 2] for k in range(5)]
    pair_loop(list_a, list_b, 0, stop, feat_f, feat_g, acc, n * rows // 16, pairs)
    for k in range(n):
        for r in range(3):
            outs[k][pl.ds(r * tiles, tiles), :] = acc[pl.ds(k * rows + r, tiles, stride=8), :]


def run_pairs(classes, tables, own_block, blocks, name):
    n = len(classes)
    tiles = own_block.shape[0] // 7
    rows = 8 * tiles
    slots = tables[0].shape[0]
    smem = pl.BlockSpec(memory_space=pltpu.SMEM)
    vmem = pl.BlockSpec(memory_space=pltpu.VMEM)
    return pl.pallas_call(
        functools.partial(kernel, classes),
        out_shape=[jax.ShapeDtypeStruct((3 * tiles, 128), F32)] * n,
        in_specs=[smem] * 4 + [vmem] * n,
        out_specs=[vmem] * n,
        scratch_shapes=[
            pltpu.VMEM((3 * rows, 128), F32),
            pltpu.VMEM((2 * n * rows, 128), F32),
            pltpu.VMEM((n * rows + 16, 128), F32),
            pltpu.SMEM((slots + 8,), jnp.int32),
            pltpu.SMEM((slots + 8,), jnp.int32),
        ]
        + [pltpu.VMEM((3, 256, 256), F32)] * 2
        + [pltpu.VMEM((6, 256, 256), BF16)] * 2
        + [pltpu.VMEM((64, 256), BF16)] * 2
        + [pltpu.VMEM((256, 128), F32)] * 2
        + [pltpu.VMEM((8, 256), F32)] * 2,
        compiler_params=pltpu.CompilerParams(
            vmem_limit_bytes=48 * 2**20,
        ),
        cost_estimate=pl.CostEstimate(
            flops=30 * 10**9, bytes_accessed=4 * 10**6, transcendentals=0
        ),
        name=name,
    )(*tables, own_block, *blocks)


LOCAL, PARTNER, OTHER, BACK, AHEAD = range(5)


def body(positions, normals, areas, pair_first, pair_second, pair_count):
    faces = areas.shape[0]
    clusters = faces // C
    tiles = faces // 128
    devices = lax.axis_size(AXES)
    me = lax.axis_index(AXES)
    odd = me % 2
    geometry = jnp.concatenate([positions, normals, areas[None, :]], axis=0)
    geometry = geometry.reshape(7, tiles, 128).transpose(1, 0, 2).reshape(7 * tiles, 128)

    def permute(x, to):
        pairs = [(i, to(i)) for i in range(devices) if 0 <= to(i) < devices]
        return lax.ppermute(x, AXES, pairs)

    def swap(x):
        return permute(x, lambda i: i ^ 1)

    delta = pair_second // clusters - me
    toward = delta * (1 - 2 * odd)
    kind = jnp.where(toward == 1, PARTNER, jnp.where(toward == -1, OTHER, LOCAL))
    kind = jnp.where(delta == -2, BACK, jnp.where(delta == 2, AHEAD, kind))
    tables = (pair_first - me * clusters, pair_second % clusters, kind, pair_count)

    back = permute(geometry, lambda i: i + 2)
    ahead = permute(geometry, lambda i: i - 2)
    partner = swap(geometry)
    own1, to_partner = run_pairs((LOCAL, PARTNER), tables, geometry, [partner], "near_pairs")
    own1, to_partner, back, ahead = lax.optimization_barrier((own1, to_partner, back, ahead))
    relay = jnp.where(odd == 1, back, ahead)
    got = swap(jnp.concatenate([relay, to_partner], axis=0))
    other, from_partner = got[: 7 * tiles], got[7 * tiles :]
    own2, to_back, to_ahead = run_pairs(
        (-1, BACK, AHEAD), tables, geometry, [back, ahead], "far_pairs"
    )
    from_ahead = permute(to_back, lambda i: i - 2)
    from_back = permute(to_ahead, lambda i: i + 2)
    own3, to_other = run_pairs((-1, OTHER), tables, geometry, [other], "other_pairs")
    from_other = permute(to_other, lambda i: i - 1 if i % 2 == 0 else i + 1)
    total = own1 + own2 + own3 + from_partner + from_ahead + from_back + from_other
    return total.reshape(3, faces)


def solution(mesh):
    in_specs = (
        P(None, AXES),
        P(None, AXES),
        P(AXES),
        P(AXES),
        P(AXES),
        P(AXES),
    )
    return jax.shard_map(
        body, mesh=mesh, in_specs=in_specs, out_specs=P(None, AXES), check_vma=False
    )
```

```python
import functools

import jax
import jax.numpy as jnp
from jax import lax
from jax.experimental import pallas as pl
from jax.experimental.pallas import tpu as pltpu
from jax.sharding import PartitionSpec as P


C = 256
AXES = ("gx", "gy")
UNROLL = 4
ROWS = 32
TABLE = 8
HEAD = 28
BALANCE = 13
F32 = jnp.float32
BF16 = jnp.bfloat16
NN = ((1,), (0,))
NT = ((1,), (1,))
TN = ((0,), (0,))


def dot(a, b, dims):
    return lax.dot_general(a, b, (dims, ((), ())), preferred_element_type=F32)


def rounded(x):
    return x.astype(BF16).astype(F32)


def two_tiles(ref, base, pitch, n):
    return jnp.concatenate([ref[pl.ds(base, n), :], ref[pl.ds(base + pitch, n), :]], axis=1)


def features(block, feat_g, g_base, feat_f, f_base):
    zero = jnp.zeros((8, 128), F32)
    one = jnp.ones((8, 128), F32)

    def step(j, carry):
        p0, p1, p2, n0, n1, n2, area = [block[pl.ds(j * 56 + k, 8, stride=7), :] for k in range(7)]
        s = jnp.exp(jnp.log(area) * (-1.0 / 3.0))
        pp = (p0 * p0 + p1 * p1 + p2 * p2 + 0.5) * s
        dot_np = n0 * p0 + n1 * p1 + n2 * p2
        q0, q1, q2 = p0 * s, p1 * s, p2 * s
        g_rows = (q0, q1, q2, pp, s, zero, zero, zero, p0, p1, p2, n0, n1, n2, dot_np, one)
        for r, v in enumerate(g_rows if feat_g is not None else ()):
            feat_g[pl.ds(g_base + j * 128 + r, 8, stride=16), :] = v
        if feat_f is not None:
            f_rows = (-2.0 * q0, -2.0 * q1, -2.0 * q2, s, pp, zero, zero, zero)
            f_rows += (-n0, -n1, -n2, zero, zero, zero, zero, dot_np)
            f_rows += (zero, zero, zero, p0, p1, p2, -one, zero)
            for r, v in enumerate(f_rows):
                feat_f[pl.ds(f_base + j * 192 + r, 8, stride=24), :] = v
        return carry

    lax.fori_loop(0, (block.shape[0] - TABLE) // 56, step, 0)


def pair_loop(lists, row, start, stop, feat_f, feat_g, acc, b_shift, dummy, scratch):
    forms, terms, weights, row_part, col_part = scratch

    def clusters(t):
        live = jnp.logical_and(t >= start, t < stop)
        safe = jnp.clip(t, start, stop - 1)
        a = lists[row, safe]
        b = lists[row + 1, safe]
        return a, b, jnp.where(live, a, dummy), jnp.where(live, b + b_shift, dummy)

    def stage(t, par):
        form_w, form_r = forms[par], forms[1 - par]
        term_w, term_r = terms[1 - par], terms[par]
        state = {}

        def prepare():
            a, b, _, _ = clusters(t)
            f = two_tiles(feat_f, pl.multiple_of(a * 48, 8), 24, 24)
            g = two_tiles(feat_g, pl.multiple_of(b * 32, 8), 16, 16)
            f1 = rounded(f)
            rest = f - f1
            f2 = rounded(rest)
            f3 = rest - f2
            g1 = rounded(g)
            rest = g - g1
            g2 = rounded(rest)
            g3 = rest - g2
            state["f"] = (f1, f2)
            state["g"] = (g1, g2)
            state["left"] = []
            for k in range(3):
                at = slice(8 * k, 8 * k + 8)
                state["left"].append(
                    jnp.concatenate([f1[at], f2[at], f3[at], f1[at], f2[at], f1[at]], axis=0)
                )
            state["right"] = []
            for k in range(2):
                at = slice(8 * k, 8 * k + 8)
                state["right"].append(
                    jnp.concatenate([g1[at], g1[at], g1[at], g2[at], g2[at], g3[at]], axis=0)
                )

        def form(k):
            def run():
                form_w[k] = dot(state["left"][k], state["right"][min(k, 1)], TN)

            return run

        def keep_weights():
            f1, f2 = state["f"]
            g1, g2 = state["g"]
            for k, (x, y) in enumerate(((f1, f2), (g1, g2))):
                for h in range(2):
                    at = slice(8 * h, 8 * h + 8)
                    rows = slice(32 * k + 16 * h, 32 * k + 16 * h + 16)
                    weights[par][rows] = jnp.concatenate([x[at], y[at]], axis=0).astype(BF16)

        col_sum = []

        def term(c):
            def run():
                rows = pl.ds(c * ROWS, ROWS)
                r2 = form_r[0, rows, :]
                sf = form_r[1, rows, :]
                sg = form_r[2, rows, :]
                inv = 1.0 / r2
                w = inv * inv * inv
                a = w * sf
                b = w * sg
                q = inv * (sf * a + sg * b)
                for m, v in enumerate((a, b, q)):
                    high = v.astype(BF16)
                    term_w[2 * m, rows, :] = high
                    term_w[2 * m + 1, rows, :] = (v - high.astype(F32)).astype(BF16)
                row_part[1 - par][rows, :] = a[:, :128] + a[:, 128:]
                part = b[0:8]
                for i in range(1, ROWS // 8):
                    part = part + b[8 * i : 8 * i + 8]
                col_sum.append(part)

            return run

        sums = {}

        def reduce(name, row, m, dims):
            def run():
                o = dot(weights[par][row : row + 16], term_r[m], dims)
                sums[name] = sums[name] + o if name in sums else o

            return run

        def plain_sums():
            turned = jnp.transpose(row_part[par][...])
            total = turned[0:8]
            for i in range(1, 16):
                total = total + turned[8 * i : 8 * i + 8]
            sums["a"] = jnp.sum(total, axis=0, keepdims=True)
            sums["b"] = jnp.sum(col_part[par][...], axis=0, keepdims=True)

        def finish():
            a, b, a_to, b_to = clusters(t - 2)

            def joined(x):
                return x[0:8] + x[8:16]

            def wide(x):
                return jnp.broadcast_to(x, (8, 256))

            col_q, col_a = joined(sums["col_q"]), joined(sums["col_a"])
            row_q, row_b = joined(sums["row_q"]), joined(sums["row_b"])
            fr = two_tiles(feat_f, pl.multiple_of(a * 48, 8), 24, 8)
            fs = two_tiles(feat_f, pl.multiple_of(a * 48 + 8, 8), 24, 8)
            gp = two_tiles(feat_g, pl.multiple_of(b * 32, 8), 16, 8)
            gq = two_tiles(feat_g, pl.multiple_of(b * 32 + 8, 8), 16, 8)
            grad_f = 3.0 * fr * wide(row_q[4:5]) + 6.0 * wide(fr[3:4]) * row_q
            grad_f = grad_f - 2.0 * fs * wide(sums["a"]) + 2.0 * pltpu.roll(row_b, 5, 0)
            grad_g = 2.0 * col_a - 2.0 * wide(sums["b"]) * pltpu.roll(gq, 5, 0)
            grad_g = grad_g - 3.0 * wide(gp[4:5]) * col_q - 6.0 * gp * wide(col_q[3:4])
            for c, g in ((a_to, grad_f), (b_to, grad_g)):
                at = pl.multiple_of(c * 16, 8)
                acc[pl.ds(at, 8), :] += g[:, :128]
                acc[pl.ds(at + 8, 8), :] += g[:, 128:]

        others = [
            prepare,
            reduce("col_a", 16, 0, NN),
            reduce("col_a", 16, 1, NN),
            form(0),
            form(1),
            form(2),
            reduce("col_q", 0, 4, NN),
            reduce("col_q", 0, 5, NN),
            reduce("row_q", 32, 4, NT),
            reduce("row_q", 32, 5, NT),
            reduce("row_b", 48, 2, NT),
            reduce("row_b", 48, 3, NT),
            plain_sums,
            finish,
            keep_weights,
        ]
        chunks = 256 // ROWS
        each = -(-len(others) // chunks)
        for c in range(chunks):
            for other in others[each * c : each * c + each]:
                other()
            term(c)()
        total = col_sum[0]
        for part in col_sum[1:]:
            total = total + part
        col_part[1 - par][...] = total

    def body(i, carry):
        for u in range(UNROLL):
            stage(start + i * UNROLL + u, u % 2)
        return carry

    trips = jnp.where(stop > start, (stop - start + 2 + UNROLL - 1) // UNROLL, 0)
    lax.fori_loop(0, trips, body, 0)


def scratch_of(rows, f_blocks, g_blocks, acc_blocks):
    return (
        [
            pltpu.VMEM((3 * f_blocks * rows, 128), F32),
            pltpu.VMEM((2 * g_blocks * rows, 128), F32),
            pltpu.VMEM((acc_blocks * rows + 16, 128), F32),
        ]
        + [pltpu.VMEM((3, 256, 256), F32)] * 2
        + [pltpu.VMEM((6, 256, 256), BF16)] * 2
        + [pltpu.VMEM((64, 256), BF16)] * 2
        + [pltpu.VMEM((256, 128), F32)] * 2
        + [pltpu.VMEM((8, 256), F32)] * 2
    )


def by_stage(scratch):
    return [scratch[2 * k : 2 * k + 2] for k in range(5)]


def compact(acc, k, r, rows):
    return acc[pl.ds(k * rows + r, rows // 8, stride=8), :]


def unpack(table, j, bits):
    code = table[j // 128, j % 128].astype(jnp.int32)
    mask = (1 << bits) - 1
    return code >> (2 * bits), code & mask, (code >> bits) & mask


def copy_table(block, table):
    pltpu.sync_copy(block.at[pl.ds(block.shape[0] - TABLE, TABLE)], table)


def append(lists, row, n, a, b, take):
    lists[row, n] = a
    lists[row + 1, n] = b
    return n + take.astype(jnp.int32)


def near_lists(odd, own, partner, lists, meta, own_table, partner_table, slots, bits):
    copy_table(own, own_table)
    copy_table(partner, partner_table)
    mine = own[pl.ds(own.shape[0] - TABLE, TABLE), :]
    its = partner[pl.ds(partner.shape[0] - TABLE, TABLE), :]
    even_codes = jnp.where(odd == 1, its, mine)
    odd_codes = jnp.where(odd == 1, mine, its)
    unit = float(1 << (2 * bits))

    def count(codes, field):
        hit = jnp.logical_and(codes >= field * unit, codes < (field + 1) * unit)
        return jnp.sum(jnp.where(hit, 1.0, 0.0)).astype(jnp.int32)

    cross_even = count(even_codes, 3)
    cross = cross_even + count(odd_codes, 1)
    odd_load = count(odd_codes, 2) + count(even_codes, 1) + count(odd_codes, 0) + BALANCE
    even_load = count(even_codes, 2) + count(even_codes, 0)
    at_even = jnp.clip((odd_load - even_load + cross) // 2, 0, cross)
    even_cut = jnp.minimum(at_even, cross_even)
    odd_cut = at_even - even_cut
    own_cut = jnp.where(odd == 1, odd_cut, even_cut)
    partner_cut = jnp.where(odd == 1, even_cut, odd_cut)
    own_cross = jnp.where(odd == 1, 1, 3)
    partner_cross = 4 - own_cross
    clusters = 1 << bits

    def step(j, carry):
        near, far, k_own, k_partner = carry
        field, f, g = unpack(own_table, j, bits)
        is_cross = field == own_cross
        mine_too = jnp.logical_xor(k_own < own_cut, odd == 1)
        take = jnp.logical_or(field == 2, jnp.logical_and(is_cross, mine_too))
        near = append(lists, 0, near, f, g + jnp.where(is_cross, clusters, 0), take)
        far = append(lists, 2, far, f, g, field == 0)
        k_own = k_own + is_cross.astype(jnp.int32)
        field, f, g = unpack(partner_table, j, bits)
        is_cross = field == partner_cross
        mine_too = jnp.logical_xor(k_partner < partner_cut, odd == 1)
        near = append(lists, 0, near, g, f + clusters, jnp.logical_and(is_cross, mine_too))
        far = append(
            lists, 2, far, f + clusters, g, jnp.logical_and(field == 1, odd == 1)
        )
        k_partner = k_partner + is_cross.astype(jnp.int32)
        return near, far, k_own, k_partner

    near, far, _, _ = lax.fori_loop(0, slots, step, (0, 0, 0, 0), unroll=4)
    meta[0] = near
    meta[1] = far
    return near


def near_kernel(slots, bits, odd, own, partner, own_out, partner_out, lists, meta, *scratch):
    own_table, partner_table, feat_f, feat_g, acc = scratch[:5]
    rows = 8 * ((own.shape[0] - TABLE) // 7)
    near = near_lists(odd[0], own, partner, lists, meta, own_table, partner_table, slots, bits)
    acc[...] = jnp.zeros_like(acc)
    features(own, feat_g, 0, feat_f, 0)
    features(partner, feat_g, 2 * rows, None, 0)
    pair_loop(
        lists, 0, 0, jnp.minimum(near, HEAD), feat_f, feat_g, acc, 0, rows // 8, by_stage(scratch[5:])
    )
    for k, out in enumerate((own_out, partner_out)):
        for r in range(3):
            out[pl.ds(r * (rows // 8), rows // 8), :] = compact(acc, k, r, rows)


def far_kernel(slots, bits, odd, meta, lists_in, own, partner, back, o0, o1, o2, *scratch):
    outs = (o0, o1, o2)
    lists, back_table, feat_f, feat_g, acc = scratch[:5]
    rows = 8 * ((own.shape[0] - TABLE) // 7)
    clusters = 1 << bits
    copy_table(back, back_table)
    known = meta[1]

    def carry_over(j, carry):
        lists[0, j] = lists_in[2, j]
        lists[1, j] = lists_in[3, j]
        return carry

    lax.fori_loop(0, known, carry_over, 0)

    def step(j, n):
        field, f, g = unpack(back_table, j, bits)
        crossed = jnp.logical_and(field == 3, odd[0] == 1)
        a = g + jnp.where(crossed, clusters, 0)
        return append(lists, 0, n, a, f, jnp.logical_or(field == 4, crossed))

    stop = lax.fori_loop(0, slots, step, known, unroll=4)
    acc[...] = jnp.zeros_like(acc)
    features(own, None, 0, feat_f, 0)
    features(back, feat_g, 0, None, 0)

    @pl.when(odd[0] == 1)
    def _():
        features(partner, None, 0, feat_f, 3 * rows)

    pair_loop(
        lists, 0, 0, stop, feat_f, feat_g, acc, 2 * (rows // 16), 3 * (rows // 16), by_stage(scratch[5:])
    )
    for k in range(3):
        for r in range(3):
            outs[k][pl.ds(r * (rows // 8), rows // 8), :] = compact(acc, k, r, rows)


def rest_kernel(
    meta, lists, own, partner, own_1, partner_1, own_2, partner_2, own_out, partner_out, *scratch
):
    feat_f, feat_g, acc = scratch[:3]
    rows = 8 * ((own.shape[0] - TABLE) // 7)
    tiles = rows // 8
    near = meta[0]

    @pl.when(near > HEAD)
    def _():
        acc[...] = jnp.zeros_like(acc)
        features(own, feat_g, 0, feat_f, 0)
        features(partner, feat_g, 2 * rows, None, 0)

    pair_loop(
        lists, 0, HEAD, near, feat_f, feat_g, acc, 0, rows // 8, by_stage(scratch[3:])
    )
    sums = ((own_out, own_1, own_2), (partner_out, partner_1, partner_2))
    for k, (out, first, second) in enumerate(sums):
        out[...] = first[...] + second[...]

        @pl.when(near > HEAD)
        def _():
            for r in range(3):
                at = pl.ds(r * tiles, tiles)
                out[at, :] += compact(acc, k, r, rows)


def call(function, ins, out_shape, scratch, smem_in, smem_out):
    smem = pl.BlockSpec(memory_space=pltpu.SMEM)
    vmem = pl.BlockSpec(memory_space=pltpu.VMEM)
    return pl.pallas_call(
        function,
        out_shape=out_shape,
        in_specs=[smem if k < smem_in else vmem for k in range(len(ins))],
        out_specs=[vmem] * (len(out_shape) - smem_out) + [smem] * smem_out,
        scratch_shapes=scratch,
        compiler_params=pltpu.CompilerParams(vmem_limit_bytes=40 * 2**20),
        cost_estimate=pl.CostEstimate(
            flops=30 * 10**9, bytes_accessed=4 * 10**6, transcendentals=0
        ),
    )(*ins)


def body(positions, normals, areas, pair_first, pair_second, pair_count):
    faces = areas.shape[0]
    clusters = faces // C
    bits = (clusters - 1).bit_length()
    tiles = faces // 128
    rows = 8 * tiles
    slots = pair_first.shape[0]
    devices = lax.axis_size(AXES)
    me = lax.axis_index(AXES)
    odd = jnp.reshape(me % 2, (1,))

    field = pair_second // clusters - me + 2
    code = (field << (2 * bits)) + ((pair_second % clusters) << bits) + pair_first % clusters
    live = jnp.arange(slots, dtype=jnp.int32) < pair_count[0]
    code = jnp.where(live, code, -1).astype(F32)
    code = jnp.pad(code, (0, TABLE * 128 - slots), constant_values=-1.0).reshape(TABLE, 128)
    geometry = jnp.concatenate([positions, normals, areas[None, :]], axis=0)
    geometry = geometry.reshape(7, tiles, 128).transpose(1, 0, 2).reshape(7 * tiles, 128)
    block = jnp.concatenate([geometry, code], axis=0)

    def permute(x, to):
        pairs = [(i, to(i)) for i in range(devices) if 0 <= to(i) < devices]
        return lax.ppermute(x, AXES, pairs)

    back = permute(block, lambda i: i + 2)
    partner = permute(block, lambda i: i ^ 1)
    part = jax.ShapeDtypeStruct((3 * tiles, 128), F32)
    lists = jax.ShapeDtypeStruct((4, 2 * slots + 8), jnp.int32)
    tables = [pltpu.SMEM((TABLE, 128), F32)]
    own_1, partner_1, lists, meta = call(
        functools.partial(near_kernel, slots, bits),
        (odd, block, partner),
        [part, part, lists, jax.ShapeDtypeStruct((2,), jnp.int32)],
        tables * 2 + scratch_of(rows, 1, 2, 2),
        1,
        2,
    )
    own_2, partner_2, back_2 = call(
        functools.partial(far_kernel, slots, bits),
        (odd, meta, lists, block, partner, back),
        [part] * 3,
        [pltpu.SMEM((2, 3 * slots + 8), jnp.int32)] + tables + scratch_of(rows, 2, 1, 3),
        3,
        0,
    )
    ahead_sum = permute(back_2, lambda i: i - 2)
    own_sum, partner_sum = call(
        rest_kernel,
        (meta, lists, block, partner, own_1, partner_1, own_2, partner_2),
        [part, part],
        scratch_of(rows, 1, 2, 2),
        2,
        0,
    )
    total = own_sum + permute(partner_sum, lambda i: i ^ 1) + ahead_sum
    return total.reshape(3, faces)


def solution(mesh):
    in_specs = (
        P(None, AXES),
        P(None, AXES),
        P(AXES),
        P(AXES),
        P(AXES),
        P(AXES),
    )
    return jax.shard_map(
        body, mesh=mesh, in_specs=in_specs, out_specs=P(None, AXES), check_vma=False
    )
```

```python
import functools

import jax
import jax.numpy as jnp
from jax import lax
from jax.experimental import pallas as pl
from jax.experimental.pallas import tpu as pltpu
from jax.sharding import PartitionSpec as P


C = 256
AXES = ("gx", "gy")
UNROLL = 4
ROWS = 32
TABLE = 8
HEAD = 28
BALANCE = 13
F32 = jnp.float32
BF16 = jnp.bfloat16
NN = ((1,), (0,))
NT = ((1,), (1,))
TN = ((0,), (0,))


def dot(a, b, dims):
    return lax.dot_general(a, b, (dims, ((), ())), preferred_element_type=F32)


def rounded(x):
    return x.astype(BF16).astype(F32)


def two_tiles(ref, base, pitch, n):
    return jnp.concatenate([ref[pl.ds(base, n), :], ref[pl.ds(base + pitch, n), :]], axis=1)


def features(block, feat_g, g_base, feat_f, f_base):
    zero = jnp.zeros((8, 128), F32)
    one = jnp.ones((8, 128), F32)

    def step(j, carry):
        p0, p1, p2, n0, n1, n2, area = [block[pl.ds(j * 56 + k, 8, stride=7), :] for k in range(7)]
        s = jnp.exp(jnp.log(area) * (-1.0 / 3.0))
        pp = (p0 * p0 + p1 * p1 + p2 * p2 + 0.5) * s
        dot_np = n0 * p0 + n1 * p1 + n2 * p2
        q0, q1, q2 = p0 * s, p1 * s, p2 * s
        g_rows = (q0, q1, q2, pp, s, zero, zero, zero, p0, p1, p2, n0, n1, n2, dot_np, one)
        for r, v in enumerate(g_rows if feat_g is not None else ()):
            feat_g[pl.ds(g_base + j * 128 + r, 8, stride=16), :] = v
        if feat_f is not None:
            f_rows = (-2.0 * q0, -2.0 * q1, -2.0 * q2, s, pp, zero, zero, zero)
            f_rows += (-n0, -n1, -n2, zero, zero, zero, zero, dot_np)
            f_rows += (zero, zero, zero, p0, p1, p2, -one, zero)
            for r, v in enumerate(f_rows):
                feat_f[pl.ds(f_base + j * 192 + r, 8, stride=24), :] = v
        return carry

    lax.fori_loop(0, (block.shape[0] - TABLE) // 56, step, 0)


def pair_loop(lookup, start, stop, feat_f, feat_g, acc, b_shift, dummy, scratch):
    forms, terms, weights, row_part, col_part = scratch

    def clusters(t):
        live = jnp.logical_and(t >= start, t < stop)
        safe = jnp.clip(t, start, stop - 1)
        a, b = lookup(safe)
        return a, b, jnp.where(live, a, dummy), jnp.where(live, b + b_shift, dummy)

    def stage(t, par):
        form_w, form_r = forms[par], forms[1 - par]
        term_w, term_r = terms[1 - par], terms[par]
        state = {}

        def prepare():
            a, b, _, _ = clusters(t)
            f = two_tiles(feat_f, pl.multiple_of(a * 48, 8), 24, 24)
            g = two_tiles(feat_g, pl.multiple_of(b * 32, 8), 16, 16)
            f1 = rounded(f)
            rest = f - f1
            f2 = rounded(rest)
            f3 = rest - f2
            g1 = rounded(g)
            rest = g - g1
            g2 = rounded(rest)
            g3 = rest - g2
            state["f"] = (f1, f2)
            state["g"] = (g1, g2)
            state["left"] = []
            for k in range(3):
                at = slice(8 * k, 8 * k + 8)
                state["left"].append(
                    jnp.concatenate([f1[at], f2[at], f3[at], f1[at], f2[at], f1[at]], axis=0)
                )
            state["right"] = []
            for k in range(2):
                at = slice(8 * k, 8 * k + 8)
                state["right"].append(
                    jnp.concatenate([g1[at], g1[at], g1[at], g2[at], g2[at], g3[at]], axis=0)
                )

        def form(k):
            def run():
                form_w[k] = dot(state["left"][k], state["right"][min(k, 1)], TN)

            return run

        def keep_weights():
            f1, f2 = state["f"]
            g1, g2 = state["g"]
            for k, (x, y) in enumerate(((f1, f2), (g1, g2))):
                for h in range(2):
                    at = slice(8 * h, 8 * h + 8)
                    rows = slice(32 * k + 16 * h, 32 * k + 16 * h + 16)
                    weights[par][rows] = jnp.concatenate([x[at], y[at]], axis=0).astype(BF16)

        col_sum = []

        def term(c):
            def run():
                rows = pl.ds(c * ROWS, ROWS)
                r2 = form_r[0, rows, :]
                sf = form_r[1, rows, :]
                sg = form_r[2, rows, :]
                inv = 1.0 / r2
                w = inv * inv * inv
                a = w * sf
                b = w * sg
                q = inv * (sf * a + sg * b)
                for m, v in enumerate((a, b, q)):
                    high = v.astype(BF16)
                    term_w[2 * m, rows, :] = high
                    term_w[2 * m + 1, rows, :] = (v - high.astype(F32)).astype(BF16)
                row_part[1 - par][rows, :] = a[:, :128] + a[:, 128:]
                part = b[0:8]
                for i in range(1, ROWS // 8):
                    part = part + b[8 * i : 8 * i + 8]
                col_sum.append(part)

            return run

        sums = {}

        def reduce(name, row, m, dims):
            def run():
                o = dot(weights[par][row : row + 16], term_r[m], dims)
                sums[name] = sums[name] + o if name in sums else o

            return run

        def plain_sums():
            turned = jnp.transpose(row_part[par][...])
            total = turned[0:8]
            for i in range(1, 16):
                total = total + turned[8 * i : 8 * i + 8]
            sums["a"] = jnp.sum(total, axis=0, keepdims=True)
            sums["b"] = jnp.sum(col_part[par][...], axis=0, keepdims=True)

        def finish():
            a, b, a_to, b_to = clusters(t - 2)

            def joined(x):
                return x[0:8] + x[8:16]

            def wide(x):
                return jnp.broadcast_to(x, (8, 256))

            col_q, col_a = joined(sums["col_q"]), joined(sums["col_a"])
            row_q, row_b = joined(sums["row_q"]), joined(sums["row_b"])
            fr = two_tiles(feat_f, pl.multiple_of(a * 48, 8), 24, 8)
            fs = two_tiles(feat_f, pl.multiple_of(a * 48 + 8, 8), 24, 8)
            gp = two_tiles(feat_g, pl.multiple_of(b * 32, 8), 16, 8)
            gq = two_tiles(feat_g, pl.multiple_of(b * 32 + 8, 8), 16, 8)
            grad_f = 3.0 * fr * wide(row_q[4:5]) + 6.0 * wide(fr[3:4]) * row_q
            grad_f = grad_f - 2.0 * fs * wide(sums["a"]) + 2.0 * pltpu.roll(row_b, 5, 0)
            grad_g = 2.0 * col_a - 2.0 * wide(sums["b"]) * pltpu.roll(gq, 5, 0)
            grad_g = grad_g - 3.0 * wide(gp[4:5]) * col_q - 6.0 * gp * wide(col_q[3:4])
            for c, g in ((a_to, grad_f), (b_to, grad_g)):
                at = pl.multiple_of(c * 16, 8)
                acc[pl.ds(at, 8), :] += g[:, :128]
                acc[pl.ds(at + 8, 8), :] += g[:, 128:]

        others = [
            reduce("row_q", 32, 4, NT),
            reduce("row_q", 32, 5, NT),
            reduce("row_b", 48, 2, NT),
            reduce("row_b", 48, 3, NT),
            reduce("col_a", 16, 0, NN),
            reduce("col_a", 16, 1, NN),
            reduce("col_q", 0, 4, NN),
            reduce("col_q", 0, 5, NN),
            prepare,
            form(0),
            form(1),
            form(2),
            plain_sums,
            finish,
            keep_weights,
        ]
        chunks = 256 // ROWS
        each = -(-len(others) // chunks)
        for c in range(chunks):
            for other in others[each * c : each * c + each]:
                other()
            term(c)()
        total = col_sum[0]
        for part in col_sum[1:]:
            total = total + part
        col_part[1 - par][...] = total

    def body(i, carry):
        for u in range(UNROLL):
            stage(start + i * UNROLL + u, u % 2)
        return carry

    trips = jnp.where(stop > start, (stop - start + 2 + UNROLL - 1) // UNROLL, 0)
    lax.fori_loop(0, trips, body, 0)


def scratch_of(rows, acc_blocks):
    return (
        [pltpu.VMEM((acc_blocks * rows + 16, 128), F32)]
        + [pltpu.VMEM((3, 256, 256), F32)] * 2
        + [pltpu.VMEM((6, 256, 256), BF16)] * 2
        + [pltpu.VMEM((64, 256), BF16)] * 2
        + [pltpu.VMEM((256, 128), F32)] * 2
        + [pltpu.VMEM((8, 256), F32)] * 2
    )


def by_stage(scratch):
    return [scratch[2 * k : 2 * k + 2] for k in range(5)]


def compact(acc, k, r, rows):
    return acc[pl.ds(k * rows + r, rows // 8, stride=8), :]


def sort_kernel(unit, code_ref, out):
    code = code_ref[...]
    slots = code.shape[1]
    shape = (slots, slots)
    column = jnp.transpose(jnp.broadcast_to(code, (8, slots)))[:, 0:1]
    lane = lax.broadcasted_iota(jnp.int32, shape, 1).astype(F32)
    sublane = lax.broadcasted_iota(jnp.int32, shape, 0).astype(F32)
    field_row = jnp.floor(jnp.broadcast_to(code, shape) * (1.0 / unit))
    field_column = jnp.floor(jnp.broadcast_to(column, shape) * (1.0 / unit))
    before = field_row * slots + lane < field_column * slots + sublane
    rank = jnp.sum(jnp.where(before, 1.0, 0.0), axis=1, keepdims=True)
    ordered = jnp.sum(jnp.where(rank == lane, column, 0.0), axis=0, keepdims=True)
    starts = jnp.sum(jnp.where(field_column < lane, 1.0, 0.0), axis=0, keepdims=True)
    out[...] = jnp.zeros_like(out)
    for r in range(slots // 128):
        out[r : r + 1, :] = ordered[:, 128 * r : 128 * r + 128]
    out[slots // 128 : slots // 128 + 1, :] = starts[:, :128]


def table_copies(blocks, table, sems):
    copies = []
    for k, block in enumerate(blocks):
        part = block.at[pl.ds(block.shape[0] - TABLE, TABLE)]
        copies.append(
            pltpu.make_async_copy(part, table.at[pl.ds(k * TABLE, TABLE)], sems.at[k])
        )
    for copy in copies:
        copy.start()
    return copies


def starts_of(table, k, slots):
    row = k * TABLE + slots // 128
    return [table[row, i].astype(jnp.int32) for i in range(6)]


def planner(table, bits, segments):
    mask = (1 << bits) - 1
    ends = []
    total = 0
    for length, *_ in segments:
        total = total + length
        ends.append(total)

    def lookup(t):
        _, base, swapped, a_add, b_add = segments[0]
        shift = base
        for k in range(1, len(segments)):
            _, base, swap_k, a_k, b_k = segments[k]
            past = t >= ends[k - 1]
            shift = jnp.where(past, base - ends[k - 1], shift)
            swapped = jnp.where(past, swap_k, swapped)
            a_add = jnp.where(past, a_k, a_add)
            b_add = jnp.where(past, b_k, b_add)
        at = t + shift
        code = table[at >> 7, at & 127].astype(jnp.int32)
        f = code & mask
        g = (code >> bits) & mask
        return jnp.where(swapped == 1, g, f) + a_add, jnp.where(swapped == 1, f, g) + b_add

    return lookup, total


def near_plan(odd, table, slots, bits):
    mine = starts_of(table, 0, slots)
    its = starts_of(table, 1, slots)
    even = [jnp.where(odd == 1, y, x) for x, y in zip(mine, its)]
    odds = [jnp.where(odd == 1, x, y) for x, y in zip(mine, its)]

    def count(starts, field):
        return starts[field + 1] - starts[field]

    cross_even = count(even, 3)
    cross_odd = count(odds, 1)
    cross = cross_even + cross_odd
    odd_load = count(odds, 2) + count(even, 1) + count(odds, 0) + BALANCE
    even_load = count(even, 2) + count(even, 0)
    at_even = jnp.clip((odd_load - even_load + cross) // 2, 0, cross)
    even_cut = jnp.minimum(at_even, cross_even)
    odd_cut = at_even - even_cut
    far_table = TABLE * 128
    clusters = 1 << bits
    own_at = jnp.where(odd == 1, mine[1] + odd_cut, mine[3])
    own_len = jnp.where(odd == 1, cross_odd - odd_cut, even_cut)
    its_at = jnp.where(odd == 1, its[3] + even_cut, its[1])
    its_len = jnp.where(odd == 1, cross_even - even_cut, odd_cut)
    return planner(
        table,
        bits,
        [
            (count(mine, 2), mine[2], 0, 0, 0),
            (own_len, own_at, 0, 0, clusters),
            (its_len, its_at + far_table, 1, 0, clusters),
        ],
    )


def near_kernel(slots, bits, odd, own, partner, own_out, partner_out, feat_f, feat_g, *scratch):
    table, sems, acc = scratch[:3]
    rows = 8 * ((own.shape[0] - TABLE) // 7)
    copies = table_copies((own, partner), table, sems)
    features(own, feat_g, 0, feat_f, 0)
    features(partner, feat_g, 2 * rows, feat_f, 3 * rows)
    acc[...] = jnp.zeros_like(acc)
    for copy in copies:
        copy.wait()
    lookup, near = near_plan(odd[0], table, slots, bits)
    stop = jnp.minimum(near, HEAD)
    pair_loop(lookup, 0, stop, feat_f, feat_g, acc, 0, rows // 8, by_stage(scratch[3:]))
    for k, out in enumerate((own_out, partner_out)):
        for r in range(3):
            out[pl.ds(r * (rows // 8), rows // 8), :] = compact(acc, k, r, rows)


def far_kernel(slots, bits, odd_ref, own, partner, back, feat_f, o0, o1, o2, *scratch):
    table, sems, feat_g, acc = scratch[:4]
    rows = 8 * ((own.shape[0] - TABLE) // 7)
    copies = table_copies((own, partner, back), table, sems)
    features(back, feat_g, 0, None, 0)
    acc[...] = jnp.zeros_like(acc)
    for copy in copies:
        copy.wait()
    odd = odd_ref[0]
    mine, its, theirs = [starts_of(table, k, slots) for k in range(3)]
    unit = TABLE * 128
    clusters = 1 << bits
    lookup, far = planner(
        table,
        bits,
        [
            (mine[1], 0, 0, 0, 0),
            (odd * (its[2] - its[1]), its[1] + unit, 0, clusters, 0),
            (theirs[5] - theirs[4], theirs[4] + 2 * unit, 1, 0, 0),
            (odd * (theirs[4] - theirs[3]), theirs[3] + 2 * unit, 1, clusters, 0),
        ],
    )
    pair_loop(
        lookup, 0, far, feat_f, feat_g, acc, rows // 8, 3 * (rows // 16), by_stage(scratch[4:])
    )
    for k, out in enumerate((o0, o1, o2)):
        for r in range(3):
            out[pl.ds(r * (rows // 8), rows // 8), :] = compact(acc, k, r, rows)


def rest_kernel(
    slots, bits, odd, own, partner, feat_f, feat_g, own_1, partner_1, own_2, partner_2, own_out, partner_out, *scratch
):
    table, sems, acc = scratch[:3]
    rows = 8 * ((own.shape[0] - TABLE) // 7)
    tiles = rows // 8
    copies = table_copies((own, partner), table, sems)
    sums = ((own_out, own_1, own_2), (partner_out, partner_1, partner_2))
    for out, first, second in sums:
        out[...] = first[...] + second[...]
    for copy in copies:
        copy.wait()
    lookup, near = near_plan(odd[0], table, slots, bits)

    @pl.when(near > HEAD)
    def _():
        acc[...] = jnp.zeros_like(acc)
        pair_loop(lookup, HEAD, near, feat_f, feat_g, acc, 0, rows // 8, by_stage(scratch[3:]))
        for k, (out, _, _) in enumerate(sums):
            for r in range(3):
                out[pl.ds(r * tiles, tiles), :] += compact(acc, k, r, rows)


def call(function, ins, out_shape, scratch, smem_in=1):
    smem = pl.BlockSpec(memory_space=pltpu.SMEM)
    vmem = pl.BlockSpec(memory_space=pltpu.VMEM)
    return pl.pallas_call(
        function,
        out_shape=out_shape,
        in_specs=[smem if k < smem_in else vmem for k in range(len(ins))],
        out_specs=[vmem] * len(out_shape),
        scratch_shapes=scratch,
        compiler_params=pltpu.CompilerParams(vmem_limit_bytes=40 * 2**20),
        cost_estimate=pl.CostEstimate(
            flops=30 * 10**9, bytes_accessed=4 * 10**6, transcendentals=0
        ),
    )(*ins)


def body(positions, normals, areas, pair_first, pair_second, pair_count):
    faces = areas.shape[0]
    clusters = faces // C
    bits = (clusters - 1).bit_length()
    tiles = faces // 128
    rows = 8 * tiles
    slots = pair_first.shape[0]
    devices = lax.axis_size(AXES)
    me = lax.axis_index(AXES)
    odd = jnp.reshape(me % 2, (1,))

    field = pair_second // clusters - me + 2
    code = (field << (2 * bits)) + ((pair_second % clusters) << bits) + pair_first % clusters
    unit = float(1 << (2 * bits))
    live = jnp.arange(slots, dtype=jnp.int32) < pair_count[0]
    code = jnp.where(live, code.astype(F32), 5.0 * unit).reshape(1, slots)
    (table,) = call(
        functools.partial(sort_kernel, unit),
        (code,),
        [jax.ShapeDtypeStruct((TABLE, 128), F32)],
        [],
        0,
    )
    geometry = jnp.concatenate([positions, normals, areas[None, :]], axis=0)
    geometry = geometry.reshape(7, tiles, 128).transpose(1, 0, 2).reshape(7 * tiles, 128)
    block = jnp.concatenate([geometry, table], axis=0)

    def permute(x, to):
        pairs = [(i, to(i)) for i in range(devices) if 0 <= to(i) < devices]
        return lax.ppermute(x, AXES, pairs)

    back = permute(block, lambda i: i + 2)
    partner = permute(block, lambda i: i ^ 1)
    part = jax.ShapeDtypeStruct((3 * tiles, 128), F32)
    f_rows = jax.ShapeDtypeStruct((6 * rows, 128), F32)
    g_rows = jax.ShapeDtypeStruct((4 * rows, 128), F32)

    def tables(count):
        return [pltpu.SMEM((count * TABLE, 128), F32), pltpu.SemaphoreType.DMA((count,))]

    own_1, partner_1, feat_f, feat_g = call(
        functools.partial(near_kernel, slots, bits),
        (odd, block, partner),
        [part, part, f_rows, g_rows],
        tables(2) + scratch_of(rows, 2),
    )
    own_2, partner_2, back_2 = call(
        functools.partial(far_kernel, slots, bits),
        (odd, block, partner, back, feat_f),
        [part] * 3,
        tables(3) + [pltpu.VMEM((2 * rows, 128), F32)] + scratch_of(rows, 3),
    )
    ahead_sum = permute(back_2, lambda i: i - 2)
    own_sum, partner_sum = call(
        functools.partial(rest_kernel, slots, bits),
        (odd, block, partner, feat_f, feat_g, own_1, partner_1, own_2, partner_2),
        [part, part],
        tables(2) + scratch_of(rows, 2),
    )
    total = own_sum + permute(partner_sum, lambda i: i ^ 1) + ahead_sum
    return total.reshape(3, faces)


def solution(mesh):
    in_specs = (
        P(None, AXES),
        P(None, AXES),
        P(AXES),
        P(AXES),
        P(AXES),
        P(AXES),
    )
    return jax.shard_map(
        body, mesh=mesh, in_specs=in_specs, out_specs=P(None, AXES), check_vma=False
    )
```

```python
import functools

import jax
import jax.numpy as jnp
from jax import lax
from jax.experimental import pallas as pl
from jax.experimental.pallas import tpu as pltpu
from jax.sharding import PartitionSpec as P


C = 256
AXES = ("gx", "gy")
UNROLL = 4
FAR_UNROLL = 12
ROWS = 32
TABLE = 8
HEAD = 28
BALANCE = 13
F32 = jnp.float32
BF16 = jnp.bfloat16
NN = ((1,), (0,))
NT = ((1,), (1,))
TN = ((0,), (0,))


def dot(a, b, dims):
    return lax.dot_general(a, b, (dims, ((), ())), preferred_element_type=F32)


def rounded(x):
    return x.astype(BF16).astype(F32)


def two_tiles(ref, base, pitch, n):
    return jnp.concatenate([ref[pl.ds(base, n), :], ref[pl.ds(base + pitch, n), :]], axis=1)


def features(block, feat_g, g_base, feat_f, f_base):
    zero = jnp.zeros((8, 128), F32)
    one = jnp.ones((8, 128), F32)

    def step(j, carry):
        p0, p1, p2, n0, n1, n2, area = [block[pl.ds(j * 56 + k, 8, stride=7), :] for k in range(7)]
        s = jnp.exp(jnp.log(area) * (-1.0 / 3.0))
        pp = (p0 * p0 + p1 * p1 + p2 * p2 + 0.5) * s
        dot_np = n0 * p0 + n1 * p1 + n2 * p2
        q0, q1, q2 = p0 * s, p1 * s, p2 * s
        g_rows = (q0, q1, q2, pp, s, zero, zero, zero, p0, p1, p2, n0, n1, n2, dot_np, one)
        for r, v in enumerate(g_rows if feat_g is not None else ()):
            feat_g[pl.ds(g_base + j * 128 + r, 8, stride=16), :] = v
        if feat_f is not None:
            f_rows = (-2.0 * q0, -2.0 * q1, -2.0 * q2, s, pp, zero, zero, zero)
            f_rows += (-n0, -n1, -n2, zero, zero, zero, zero, dot_np)
            f_rows += (zero, zero, zero, p0, p1, p2, -one, zero)
            for r, v in enumerate(f_rows):
                feat_f[pl.ds(f_base + j * 192 + r, 8, stride=24), :] = v
        return carry

    lax.fori_loop(0, (block.shape[0] - TABLE) // 56, step, 0)


def pair_loop(lookup, start, stop, feat_f, feat_g, acc, b_shift, dummy, scratch, unroll=UNROLL):
    forms, terms, weights, row_part, col_part = scratch

    def clusters(t):
        live = jnp.logical_and(t >= start, t < stop)
        safe = jnp.clip(t, start, stop - 1)
        a, b = lookup(safe)
        return a, b, jnp.where(live, a, dummy), jnp.where(live, b + b_shift, dummy)

    def stage(t, par):
        form_w, form_r = forms[par], forms[1 - par]
        term_w, term_r = terms[1 - par], terms[par]
        state = {}

        def prepare():
            a, b, _, _ = clusters(t)
            f = two_tiles(feat_f, pl.multiple_of(a * 48, 8), 24, 24)
            g = two_tiles(feat_g, pl.multiple_of(b * 32, 8), 16, 16)
            f1 = rounded(f)
            rest = f - f1
            f2 = rounded(rest)
            f3 = rest - f2
            g1 = rounded(g)
            rest = g - g1
            g2 = rounded(rest)
            g3 = rest - g2
            state["f"] = (f1, f2)
            state["g"] = (g1, g2)
            state["left"] = []
            for k in range(3):
                at = slice(8 * k, 8 * k + 8)
                state["left"].append(
                    jnp.concatenate([f1[at], f2[at], f3[at], f1[at], f2[at], f1[at]], axis=0)
                )
            state["right"] = []
            for k in range(2):
                at = slice(8 * k, 8 * k + 8)
                state["right"].append(
                    jnp.concatenate([g1[at], g1[at], g1[at], g2[at], g2[at], g3[at]], axis=0)
                )

        def form(k):
            def run():
                form_w[k] = dot(state["left"][k], state["right"][min(k, 1)], TN)

            return run

        def keep_weights():
            f1, f2 = state["f"]
            g1, g2 = state["g"]
            for k, (x, y) in enumerate(((f1, f2), (g1, g2))):
                for h in range(2):
                    at = slice(8 * h, 8 * h + 8)
                    rows = slice(32 * k + 16 * h, 32 * k + 16 * h + 16)
                    weights[par][rows] = jnp.concatenate([x[at], y[at]], axis=0).astype(BF16)

        col_sum = []

        def term(c):
            def run():
                rows = pl.ds(c * ROWS, ROWS)
                r2 = form_r[0, rows, :]
                sf = form_r[1, rows, :]
                sg = form_r[2, rows, :]
                inv = 1.0 / r2
                w = inv * inv * inv
                a = w * sf
                b = w * sg
                q = inv * (sf * a + sg * b)
                for m, v in enumerate((a, b, q)):
                    high = v.astype(BF16)
                    term_w[2 * m, rows, :] = high
                    term_w[2 * m + 1, rows, :] = (v - high.astype(F32)).astype(BF16)
                row_part[1 - par][rows, :] = a[:, :128] + a[:, 128:]
                part = b[0:8]
                for i in range(1, ROWS // 8):
                    part = part + b[8 * i : 8 * i + 8]
                col_sum.append(part)

            return run

        sums = {}

        def reduce(name, row, m, dims):
            def run():
                o = dot(weights[par][row : row + 16], term_r[m], dims)
                sums[name] = sums[name] + o if name in sums else o

            return run

        def plain_sums():
            turned = jnp.transpose(row_part[par][...])
            total = turned[0:8]
            for i in range(1, 16):
                total = total + turned[8 * i : 8 * i + 8]
            sums["a"] = jnp.sum(total, axis=0, keepdims=True)
            sums["b"] = jnp.sum(col_part[par][...], axis=0, keepdims=True)

        def finish():
            a, b, a_to, b_to = clusters(t - 2)

            def joined(x):
                return x[0:8] + x[8:16]

            def wide(x):
                return jnp.broadcast_to(x, (8, 256))

            col_q, col_a = joined(sums["col_q"]), joined(sums["col_a"])
            row_q, row_b = joined(sums["row_q"]), joined(sums["row_b"])
            fr = two_tiles(feat_f, pl.multiple_of(a * 48, 8), 24, 8)
            fs = two_tiles(feat_f, pl.multiple_of(a * 48 + 8, 8), 24, 8)
            gp = two_tiles(feat_g, pl.multiple_of(b * 32, 8), 16, 8)
            gq = two_tiles(feat_g, pl.multiple_of(b * 32 + 8, 8), 16, 8)
            grad_f = 3.0 * fr * wide(row_q[4:5]) + 6.0 * wide(fr[3:4]) * row_q
            grad_f = grad_f - 2.0 * fs * wide(sums["a"]) + 2.0 * pltpu.roll(row_b, 5, 0)
            grad_g = 2.0 * col_a - 2.0 * wide(sums["b"]) * pltpu.roll(gq, 5, 0)
            grad_g = grad_g - 3.0 * wide(gp[4:5]) * col_q - 6.0 * gp * wide(col_q[3:4])
            for c, g in ((a_to, grad_f), (b_to, grad_g)):
                at = pl.multiple_of(c * 16, 8)
                acc[pl.ds(at, 8), :] += g[:, :128]
                acc[pl.ds(at + 8, 8), :] += g[:, 128:]

        others = [
            reduce("row_q", 32, 4, NT),
            reduce("row_q", 32, 5, NT),
            reduce("row_b", 48, 2, NT),
            reduce("row_b", 48, 3, NT),
            reduce("col_a", 16, 0, NN),
            reduce("col_a", 16, 1, NN),
            reduce("col_q", 0, 4, NN),
            reduce("col_q", 0, 5, NN),
            prepare,
            form(0),
            form(1),
            form(2),
            plain_sums,
            finish,
            keep_weights,
        ]
        chunks = 256 // ROWS
        each = -(-len(others) // chunks)
        for c in range(chunks):
            for other in others[each * c : each * c + each]:
                other()
            term(c)()
        total = col_sum[0]
        for part in col_sum[1:]:
            total = total + part
        col_part[1 - par][...] = total

    def stages(at, step):
        def body(i, carry):
            for u in range(step):
                stage(at + i * step + u, u % 2)
            return carry

        return body

    needed = jnp.where(stop > start, stop - start + 2, 0)
    done = 0
    if unroll > UNROLL:
        trips = needed // unroll
        lax.fori_loop(0, trips, stages(start, unroll), 0)
        done = trips * unroll
    trips = (needed - done + UNROLL - 1) // UNROLL
    lax.fori_loop(0, trips, stages(start + done, UNROLL), 0)


def scratch_of(rows, acc_blocks):
    return (
        [pltpu.VMEM((acc_blocks * rows + 16, 128), F32)]
        + [pltpu.VMEM((3, 256, 256), F32)] * 2
        + [pltpu.VMEM((6, 256, 256), BF16)] * 2
        + [pltpu.VMEM((64, 256), BF16)] * 2
        + [pltpu.VMEM((256, 128), F32)] * 2
        + [pltpu.VMEM((8, 256), F32)] * 2
    )


def by_stage(scratch):
    return [scratch[2 * k : 2 * k + 2] for k in range(5)]


def compact(acc, k, r, rows):
    return acc[pl.ds(k * rows + r, rows // 8, stride=8), :]


def sort_kernel(unit, code_ref, out):
    code = code_ref[...]
    slots = code.shape[1]
    shape = (slots, slots)
    column = jnp.transpose(jnp.broadcast_to(code, (8, slots)))[:, 0:1]
    lane = lax.broadcasted_iota(jnp.int32, shape, 1).astype(F32)
    sublane = lax.broadcasted_iota(jnp.int32, shape, 0).astype(F32)
    field_row = jnp.floor(jnp.broadcast_to(code, shape) * (1.0 / unit))
    field_column = jnp.floor(jnp.broadcast_to(column, shape) * (1.0 / unit))
    before = field_row * slots + lane < field_column * slots + sublane
    rank = jnp.sum(jnp.where(before, 1.0, 0.0), axis=1, keepdims=True)
    ordered = jnp.sum(jnp.where(rank == lane, column, 0.0), axis=0, keepdims=True)
    starts = jnp.sum(jnp.where(field_column < lane, 1.0, 0.0), axis=0, keepdims=True)
    out[...] = jnp.zeros_like(out)
    for r in range(slots // 128):
        out[r : r + 1, :] = ordered[:, 128 * r : 128 * r + 128]
    out[slots // 128 : slots // 128 + 1, :] = starts[:, :128]


def table_copies(blocks, table, sems):
    copies = []
    for k, block in enumerate(blocks):
        part = block.at[pl.ds(block.shape[0] - TABLE, TABLE)]
        copies.append(
            pltpu.make_async_copy(part, table.at[pl.ds(k * TABLE, TABLE)], sems.at[k])
        )
    for copy in copies:
        copy.start()
    return copies


def starts_of(table, k, slots):
    row = k * TABLE + slots // 128
    return [table[row, i].astype(jnp.int32) for i in range(6)]


def planner(table, bits, segments):
    mask = (1 << bits) - 1
    ends = []
    total = 0
    for length, *_ in segments:
        total = total + length
        ends.append(total)

    def lookup(t):
        _, base, swapped, a_add, b_add = segments[0]
        shift = base
        for k in range(1, len(segments)):
            _, base, swap_k, a_k, b_k = segments[k]
            past = t >= ends[k - 1]
            shift = jnp.where(past, base - ends[k - 1], shift)
            swapped = jnp.where(past, swap_k, swapped)
            a_add = jnp.where(past, a_k, a_add)
            b_add = jnp.where(past, b_k, b_add)
        at = t + shift
        code = table[at >> 7, at & 127].astype(jnp.int32)
        f = code & mask
        g = (code >> bits) & mask
        return jnp.where(swapped == 1, g, f) + a_add, jnp.where(swapped == 1, f, g) + b_add

    return lookup, total


def near_plan(odd, table, slots, bits):
    mine = starts_of(table, 0, slots)
    its = starts_of(table, 1, slots)
    even = [jnp.where(odd == 1, y, x) for x, y in zip(mine, its)]
    odds = [jnp.where(odd == 1, x, y) for x, y in zip(mine, its)]

    def count(starts, field):
        return starts[field + 1] - starts[field]

    cross_even = count(even, 3)
    cross_odd = count(odds, 1)
    cross = cross_even + cross_odd
    odd_load = count(odds, 2) + count(even, 1) + count(odds, 0) + BALANCE
    even_load = count(even, 2) + count(even, 0)
    at_even = jnp.clip((odd_load - even_load + cross) // 2, 0, cross)
    even_cut = jnp.minimum(at_even, cross_even)
    odd_cut = at_even - even_cut
    far_table = TABLE * 128
    clusters = 1 << bits
    own_at = jnp.where(odd == 1, mine[1] + odd_cut, mine[3])
    own_len = jnp.where(odd == 1, cross_odd - odd_cut, even_cut)
    its_at = jnp.where(odd == 1, its[3] + even_cut, its[1])
    its_len = jnp.where(odd == 1, cross_even - even_cut, odd_cut)
    return planner(
        table,
        bits,
        [
            (count(mine, 2), mine[2], 0, 0, 0),
            (own_len, own_at, 0, 0, clusters),
            (its_len, its_at + far_table, 1, 0, clusters),
        ],
    )


def near_kernel(slots, bits, odd, own, partner, own_out, partner_out, feat_f, feat_g, *scratch):
    table, sems, acc = scratch[:3]
    rows = 8 * ((own.shape[0] - TABLE) // 7)
    copies = table_copies((own, partner), table, sems)
    features(own, feat_g, 0, feat_f, 0)
    features(partner, feat_g, 2 * rows, feat_f, 3 * rows)
    acc[...] = jnp.zeros_like(acc)
    for copy in copies:
        copy.wait()
    lookup, near = near_plan(odd[0], table, slots, bits)
    stop = jnp.minimum(near, HEAD)
    pair_loop(lookup, 0, stop, feat_f, feat_g, acc, 0, rows // 8, by_stage(scratch[3:]))
    for k, out in enumerate((own_out, partner_out)):
        for r in range(3):
            out[pl.ds(r * (rows // 8), rows // 8), :] = compact(acc, k, r, rows)


def far_kernel(slots, bits, odd_ref, own, partner, back, feat_f, o0, o1, o2, *scratch):
    table, sems, feat_g, acc = scratch[:4]
    rows = 8 * ((own.shape[0] - TABLE) // 7)
    copies = table_copies((own, partner, back), table, sems)
    features(back, feat_g, 0, None, 0)
    acc[...] = jnp.zeros_like(acc)
    for copy in copies:
        copy.wait()
    odd = odd_ref[0]
    mine, its, theirs = [starts_of(table, k, slots) for k in range(3)]
    unit = TABLE * 128
    clusters = 1 << bits
    lookup, far = planner(
        table,
        bits,
        [
            (mine[1], 0, 0, 0, 0),
            (odd * (its[2] - its[1]), its[1] + unit, 0, clusters, 0),
            (theirs[5] - theirs[4], theirs[4] + 2 * unit, 1, 0, 0),
            (odd * (theirs[4] - theirs[3]), theirs[3] + 2 * unit, 1, clusters, 0),
        ],
    )
    pair_loop(
        lookup,
        0,
        far,
        feat_f,
        feat_g,
        acc,
        rows // 8,
        3 * (rows // 16),
        by_stage(scratch[4:]),
        FAR_UNROLL,
    )
    for k, out in enumerate((o0, o1, o2)):
        for r in range(3):
            out[pl.ds(r * (rows // 8), rows // 8), :] = compact(acc, k, r, rows)


def rest_kernel(
    slots, bits, odd, own, partner, feat_f, feat_g, own_1, partner_1, own_2, partner_2, own_out, partner_out, *scratch
):
    table, sems, acc = scratch[:3]
    rows = 8 * ((own.shape[0] - TABLE) // 7)
    tiles = rows // 8
    copies = table_copies((own, partner), table, sems)
    sums = ((own_out, own_1, own_2), (partner_out, partner_1, partner_2))
    for out, first, second in sums:
        out[...] = first[...] + second[...]
    for copy in copies:
        copy.wait()
    lookup, near = near_plan(odd[0], table, slots, bits)

    @pl.when(near > HEAD)
    def _():
        acc[...] = jnp.zeros_like(acc)
        pair_loop(lookup, HEAD, near, feat_f, feat_g, acc, 0, rows // 8, by_stage(scratch[3:]))
        for k, (out, _, _) in enumerate(sums):
            for r in range(3):
                out[pl.ds(r * tiles, tiles), :] += compact(acc, k, r, rows)


def call(function, ins, out_shape, scratch, smem_in=1, any_in=0):
    smem = pl.BlockSpec(memory_space=pltpu.SMEM)
    vmem = pl.BlockSpec(memory_space=pltpu.VMEM)
    anywhere = pl.BlockSpec(memory_space=pltpu.HBM)
    return pl.pallas_call(
        function,
        out_shape=out_shape,
        in_specs=[smem] * smem_in + [anywhere] * any_in + [vmem] * (len(ins) - smem_in - any_in),
        out_specs=[vmem] * len(out_shape),
        scratch_shapes=scratch,
        compiler_params=pltpu.CompilerParams(vmem_limit_bytes=40 * 2**20),
        cost_estimate=pl.CostEstimate(
            flops=30 * 10**9, bytes_accessed=4 * 10**6, transcendentals=0
        ),
    )(*ins)


def body(positions, normals, areas, pair_first, pair_second, pair_count):
    faces = areas.shape[0]
    clusters = faces // C
    bits = (clusters - 1).bit_length()
    tiles = faces // 128
    rows = 8 * tiles
    slots = pair_first.shape[0]
    devices = lax.axis_size(AXES)
    me = lax.axis_index(AXES)
    odd = jnp.reshape(me % 2, (1,))

    field = pair_second // clusters - me + 2
    code = (field << (2 * bits)) + ((pair_second % clusters) << bits) + pair_first % clusters
    unit = float(1 << (2 * bits))
    live = jnp.arange(slots, dtype=jnp.int32) < pair_count[0]
    code = jnp.where(live, code.astype(F32), 5.0 * unit).reshape(1, slots)
    (table,) = call(
        functools.partial(sort_kernel, unit),
        (code,),
        [jax.ShapeDtypeStruct((TABLE, 128), F32)],
        [],
        0,
    )
    geometry = jnp.concatenate([positions, normals, areas[None, :]], axis=0)
    geometry = geometry.reshape(7, tiles, 128).transpose(1, 0, 2).reshape(7 * tiles, 128)
    block = jnp.concatenate([geometry, table], axis=0)

    def permute(x, to):
        pairs = [(i, to(i)) for i in range(devices) if 0 <= to(i) < devices]
        return lax.ppermute(x, AXES, pairs)

    back = permute(block, lambda i: i + 2)
    partner = permute(block, lambda i: i ^ 1)
    part = jax.ShapeDtypeStruct((3 * tiles, 128), F32)
    f_rows = jax.ShapeDtypeStruct((6 * rows, 128), F32)
    g_rows = jax.ShapeDtypeStruct((4 * rows, 128), F32)

    def tables(count):
        return [pltpu.SMEM((count * TABLE, 128), F32), pltpu.SemaphoreType.DMA((count,))]

    own_1, partner_1, feat_f, feat_g = call(
        functools.partial(near_kernel, slots, bits),
        (odd, block, partner),
        [part, part, f_rows, g_rows],
        tables(2) + scratch_of(rows, 2),
    )
    own_2, partner_2, back_2 = call(
        functools.partial(far_kernel, slots, bits),
        (odd, block, partner, back, feat_f),
        [part] * 3,
        tables(3) + [pltpu.VMEM((2 * rows, 128), F32)] + scratch_of(rows, 3),
    )
    ahead_sum = permute(back_2, lambda i: i - 2)
    own_sum, partner_sum = call(
        functools.partial(rest_kernel, slots, bits),
        (odd, block, partner, feat_f, feat_g, own_1, partner_1, own_2, partner_2),
        [part, part],
        tables(2) + scratch_of(rows, 2),
    )
    total = own_sum + permute(partner_sum, lambda i: i ^ 1) + ahead_sum
    return total.reshape(3, faces)


def solution(mesh):
    in_specs = (
        P(None, AXES),
        P(None, AXES),
        P(AXES),
        P(AXES),
        P(AXES),
        P(AXES),
    )
    return jax.shard_map(
        body, mesh=mesh, in_specs=in_specs, out_specs=P(None, AXES), check_vma=False
    )
```

```python
import functools

import jax
import jax.numpy as jnp
from jax import lax
from jax.experimental import pallas as pl
from jax.experimental.pallas import tpu as pltpu
from jax.sharding import PartitionSpec as P


C = 256
AXES = ("gx", "gy")
UNROLL = 12
TAIL = 4
ROWS = 32
TABLE = 8
HEAD = 34
BALANCE = 13
F32 = jnp.float32
BF16 = jnp.bfloat16
NN = ((1,), (0,))
NT = ((1,), (1,))
TN = ((0,), (0,))


def dot(a, b, dims):
    return lax.dot_general(a, b, (dims, ((), ())), preferred_element_type=F32)


def rounded(x):
    return x.astype(BF16).astype(F32)


def two_tiles(ref, base, pitch, n):
    return jnp.concatenate([ref[pl.ds(base, n), :], ref[pl.ds(base + pitch, n), :]], axis=1)


def features(block, feat_g, g_base, feat_f, f_base):
    zero = jnp.zeros((8, 128), F32)
    one = jnp.ones((8, 128), F32)

    def step(j, carry):
        p0, p1, p2, n0, n1, n2, area = [block[pl.ds(j * 56 + k, 8, stride=7), :] for k in range(7)]
        s = jnp.exp(jnp.log(area) * (-1.0 / 3.0))
        pp = (p0 * p0 + p1 * p1 + p2 * p2 + 0.5) * s
        dot_np = n0 * p0 + n1 * p1 + n2 * p2
        q0, q1, q2 = p0 * s, p1 * s, p2 * s
        g_rows = (q0, q1, q2, pp, s, zero, zero, zero, p0, p1, p2, n0, n1, n2, dot_np, one)
        for r, v in enumerate(g_rows if feat_g is not None else ()):
            feat_g[pl.ds(g_base + j * 128 + r, 8, stride=16), :] = v
        if feat_f is not None:
            f_rows = (-2.0 * q0, -2.0 * q1, -2.0 * q2, s, pp, zero, zero, zero)
            f_rows += (-n0, -n1, -n2, zero, zero, zero, zero, dot_np)
            f_rows += (zero, zero, zero, p0, p1, p2, -one, zero)
            for r, v in enumerate(f_rows):
                feat_f[pl.ds(f_base + j * 192 + r, 8, stride=24), :] = v
        return carry

    lax.fori_loop(0, (block.shape[0] - TABLE) // 56, step, 0)


def pair_loop(lookup, start, stop, feat_f, feat_g, acc, b_shift, dummy, scratch):
    forms, terms, weights, row_part, col_part = scratch

    def clusters(t):
        live = jnp.logical_and(t >= start, t < stop)
        safe = jnp.clip(t, start, stop - 1)
        a, b = lookup(safe)
        return a, b, jnp.where(live, a, dummy), jnp.where(live, b + b_shift, dummy)

    def stage(t, par):
        form_w, form_r = forms[par], forms[1 - par]
        term_w, term_r = terms[1 - par], terms[par]
        state = {}

        def prepare():
            a, b, _, _ = clusters(t)
            f = two_tiles(feat_f, pl.multiple_of(a * 48, 8), 24, 24)
            g = two_tiles(feat_g, pl.multiple_of(b * 32, 8), 16, 16)
            f1 = rounded(f)
            rest = f - f1
            f2 = rounded(rest)
            f3 = rest - f2
            g1 = rounded(g)
            rest = g - g1
            g2 = rounded(rest)
            g3 = rest - g2
            state["f"] = (f1, f2)
            state["g"] = (g1, g2)
            state["left"] = []
            for k in range(3):
                at = slice(8 * k, 8 * k + 8)
                state["left"].append(
                    jnp.concatenate([f1[at], f2[at], f3[at], f1[at], f2[at], f1[at]], axis=0)
                )
            state["right"] = []
            for k in range(2):
                at = slice(8 * k, 8 * k + 8)
                state["right"].append(
                    jnp.concatenate([g1[at], g1[at], g1[at], g2[at], g2[at], g3[at]], axis=0)
                )

        def form(k):
            def run():
                form_w[k] = dot(state["left"][k], state["right"][min(k, 1)], TN)

            return run

        def keep_weights():
            f1, f2 = state["f"]
            g1, g2 = state["g"]
            for k, (x, y) in enumerate(((f1, f2), (g1, g2))):
                for h in range(2):
                    at = slice(8 * h, 8 * h + 8)
                    rows = slice(32 * k + 16 * h, 32 * k + 16 * h + 16)
                    weights[par][rows] = jnp.concatenate([x[at], y[at]], axis=0).astype(BF16)

        col_sum = []

        def term(c):
            def run():
                rows = pl.ds(c * ROWS, ROWS)
                r2 = form_r[0, rows, :]
                sf = form_r[1, rows, :]
                sg = form_r[2, rows, :]
                inv = 1.0 / r2
                w = inv * inv * inv
                a = w * sf
                b = w * sg
                q = inv * (sf * a + sg * b)
                for m, v in enumerate((a, b, q)):
                    high = v.astype(BF16)
                    term_w[2 * m, rows, :] = high
                    term_w[2 * m + 1, rows, :] = (v - high.astype(F32)).astype(BF16)
                row_part[1 - par][rows, :] = a[:, :128] + a[:, 128:]
                part = b[0:8]
                for i in range(1, ROWS // 8):
                    part = part + b[8 * i : 8 * i + 8]
                col_sum.append(part)

            return run

        sums = {}

        def reduce(name, row, m, dims):
            def run():
                o = dot(weights[par][row : row + 16], term_r[m], dims)
                sums[name] = sums[name] + o if name in sums else o

            return run

        def plain_sums():
            turned = jnp.transpose(row_part[par][...])
            total = turned[0:8]
            for i in range(1, 16):
                total = total + turned[8 * i : 8 * i + 8]
            sums["a"] = jnp.sum(total, axis=0, keepdims=True)
            sums["b"] = jnp.sum(col_part[par][...], axis=0, keepdims=True)

        def finish():
            a, b, a_to, b_to = clusters(t - 2)

            def joined(x):
                return x[0:8] + x[8:16]

            def wide(x):
                return jnp.broadcast_to(x, (8, 256))

            col_q, col_a = joined(sums["col_q"]), joined(sums["col_a"])
            row_q, row_b = joined(sums["row_q"]), joined(sums["row_b"])
            fr = two_tiles(feat_f, pl.multiple_of(a * 48, 8), 24, 8)
            fs = two_tiles(feat_f, pl.multiple_of(a * 48 + 8, 8), 24, 8)
            gp = two_tiles(feat_g, pl.multiple_of(b * 32, 8), 16, 8)
            gq = two_tiles(feat_g, pl.multiple_of(b * 32 + 8, 8), 16, 8)
            grad_f = 3.0 * fr * wide(row_q[4:5]) + 6.0 * wide(fr[3:4]) * row_q
            grad_f = grad_f - 2.0 * fs * wide(sums["a"]) + 2.0 * pltpu.roll(row_b, 5, 0)
            grad_g = 2.0 * col_a - 2.0 * wide(sums["b"]) * pltpu.roll(gq, 5, 0)
            grad_g = grad_g - 3.0 * wide(gp[4:5]) * col_q - 6.0 * gp * wide(col_q[3:4])
            for c, g in ((a_to, grad_f), (b_to, grad_g)):
                at = pl.multiple_of(c * 16, 8)
                acc[pl.ds(at, 8), :] += g[:, :128]
                acc[pl.ds(at + 8, 8), :] += g[:, 128:]

        others = [
            reduce("row_q", 32, 4, NT),
            reduce("row_q", 32, 5, NT),
            reduce("row_b", 48, 2, NT),
            reduce("row_b", 48, 3, NT),
            reduce("col_a", 16, 0, NN),
            reduce("col_a", 16, 1, NN),
            reduce("col_q", 0, 4, NN),
            reduce("col_q", 0, 5, NN),
            prepare,
            form(0),
            form(1),
            form(2),
            plain_sums,
            finish,
            keep_weights,
        ]
        chunks = 256 // ROWS
        each = -(-len(others) // chunks)
        for c in range(chunks):
            for other in others[each * c : each * c + each]:
                other()
            term(c)()
        total = col_sum[0]
        for part in col_sum[1:]:
            total = total + part
        col_part[1 - par][...] = total

    def stages(at, step):
        def body(i, carry):
            for u in range(step):
                stage(at + i * step + u, u % 2)
            return carry

        return body

    needed = jnp.where(stop > start, stop - start + 2, 0)
    trips = needed // UNROLL
    lax.fori_loop(0, trips, stages(start, UNROLL), 0)
    done = trips * UNROLL
    trips = (needed - done + TAIL - 1) // TAIL
    lax.fori_loop(0, trips, stages(start + done, TAIL), 0)


def scratch_of(rows, acc_blocks):
    return (
        [pltpu.VMEM((acc_blocks * rows + 16, 128), F32)]
        + [pltpu.VMEM((3, 256, 256), F32)] * 2
        + [pltpu.VMEM((6, 256, 256), BF16)] * 2
        + [pltpu.VMEM((64, 256), BF16)] * 2
        + [pltpu.VMEM((256, 128), F32)] * 2
        + [pltpu.VMEM((8, 256), F32)] * 2
    )


def by_stage(scratch):
    return [scratch[2 * k : 2 * k + 2] for k in range(5)]


def compact(acc, k, r, rows):
    return acc[pl.ds(k * rows + r, rows // 8, stride=8), :]


def sort_kernel(unit, code_ref, out):
    code = code_ref[...]
    slots = code.shape[1]
    shape = (slots, slots)
    column = jnp.transpose(jnp.broadcast_to(code, (8, slots)))[:, 0:1]
    lane = lax.broadcasted_iota(jnp.int32, shape, 1).astype(F32)
    sublane = lax.broadcasted_iota(jnp.int32, shape, 0).astype(F32)
    field_row = jnp.floor(jnp.broadcast_to(code, shape) * (1.0 / unit))
    field_column = jnp.floor(jnp.broadcast_to(column, shape) * (1.0 / unit))
    before = field_row * slots + lane < field_column * slots + sublane
    rank = jnp.sum(jnp.where(before, 1.0, 0.0), axis=1, keepdims=True)
    ordered = jnp.sum(jnp.where(rank == lane, column, 0.0), axis=0, keepdims=True)
    starts = jnp.sum(jnp.where(field_column < lane, 1.0, 0.0), axis=0, keepdims=True)
    out[...] = jnp.zeros_like(out)
    for r in range(slots // 128):
        out[r : r + 1, :] = ordered[:, 128 * r : 128 * r + 128]
    out[slots // 128 : slots // 128 + 1, :] = starts[:, :128]


def table_copies(blocks, table, sems):
    copies = []
    for k, block in enumerate(blocks):
        part = block.at[pl.ds(block.shape[0] - TABLE, TABLE)]
        copies.append(
            pltpu.make_async_copy(part, table.at[pl.ds(k * TABLE, TABLE)], sems.at[k])
        )
    for copy in copies:
        copy.start()
    return copies


def starts_of(table, k, slots):
    row = k * TABLE + slots // 128
    return [table[row, i].astype(jnp.int32) for i in range(6)]


def planner(table, bits, segments):
    mask = (1 << bits) - 1
    ends = []
    total = 0
    for length, *_ in segments:
        total = total + length
        ends.append(total)

    def lookup(t):
        _, base, swapped, a_add, b_add = segments[0]
        shift = base
        for k in range(1, len(segments)):
            _, base, swap_k, a_k, b_k = segments[k]
            past = t >= ends[k - 1]
            shift = jnp.where(past, base - ends[k - 1], shift)
            swapped = jnp.where(past, swap_k, swapped)
            a_add = jnp.where(past, a_k, a_add)
            b_add = jnp.where(past, b_k, b_add)
        at = t + shift
        code = table[at >> 7, at & 127].astype(jnp.int32)
        f = code & mask
        g = (code >> bits) & mask
        return jnp.where(swapped == 1, g, f) + a_add, jnp.where(swapped == 1, f, g) + b_add

    return lookup, total


def near_plan(odd, table, slots, bits):
    mine = starts_of(table, 0, slots)
    its = starts_of(table, 1, slots)
    even = [jnp.where(odd == 1, y, x) for x, y in zip(mine, its)]
    odds = [jnp.where(odd == 1, x, y) for x, y in zip(mine, its)]

    def count(starts, field):
        return starts[field + 1] - starts[field]

    cross_even = count(even, 3)
    cross_odd = count(odds, 1)
    cross = cross_even + cross_odd
    odd_load = count(odds, 2) + count(even, 1) + count(odds, 0) + BALANCE
    even_load = count(even, 2) + count(even, 0)
    at_even = jnp.clip((odd_load - even_load + cross) // 2, 0, cross)
    even_cut = jnp.minimum(at_even, cross_even)
    odd_cut = at_even - even_cut
    far_table = TABLE * 128
    clusters = 1 << bits
    own_at = jnp.where(odd == 1, mine[1] + odd_cut, mine[3])
    own_len = jnp.where(odd == 1, cross_odd - odd_cut, even_cut)
    its_at = jnp.where(odd == 1, its[3] + even_cut, its[1])
    its_len = jnp.where(odd == 1, cross_even - even_cut, odd_cut)
    return planner(
        table,
        bits,
        [
            (count(mine, 2), mine[2], 0, 0, 0),
            (own_len, own_at, 0, 0, clusters),
            (its_len, its_at + far_table, 1, 0, clusters),
        ],
    )


def near_kernel(slots, bits, odd, own, partner, own_out, partner_out, feat_f, feat_g, *scratch):
    table, sems, acc = scratch[:3]
    rows = 8 * ((own.shape[0] - TABLE) // 7)
    copies = table_copies((own, partner), table, sems)
    features(own, feat_g, 0, feat_f, 0)
    features(partner, feat_g, 2 * rows, feat_f, 3 * rows)
    acc[...] = jnp.zeros_like(acc)
    for copy in copies:
        copy.wait()
    lookup, near = near_plan(odd[0], table, slots, bits)
    stop = jnp.minimum(near, HEAD)
    pair_loop(lookup, 0, stop, feat_f, feat_g, acc, 0, rows // 8, by_stage(scratch[3:]))
    for k, out in enumerate((own_out, partner_out)):
        for r in range(3):
            out[pl.ds(r * (rows // 8), rows // 8), :] = compact(acc, k, r, rows)


def far_kernel(slots, bits, odd_ref, own, partner, back, feat_f, o0, o1, o2, *scratch):
    table, sems, feat_g, acc = scratch[:4]
    rows = 8 * ((own.shape[0] - TABLE) // 7)
    copies = table_copies((own, partner, back), table, sems)
    features(back, feat_g, 0, None, 0)
    acc[...] = jnp.zeros_like(acc)
    for copy in copies:
        copy.wait()
    odd = odd_ref[0]
    mine, its, theirs = [starts_of(table, k, slots) for k in range(3)]
    unit = TABLE * 128
    clusters = 1 << bits
    lookup, far = planner(
        table,
        bits,
        [
            (mine[1], 0, 0, 0, 0),
            (odd * (its[2] - its[1]), its[1] + unit, 0, clusters, 0),
            (theirs[5] - theirs[4], theirs[4] + 2 * unit, 1, 0, 0),
            (odd * (theirs[4] - theirs[3]), theirs[3] + 2 * unit, 1, clusters, 0),
        ],
    )
    pair_loop(
        lookup,
        0,
        far,
        feat_f,
        feat_g,
        acc,
        rows // 8,
        3 * (rows // 16),
        by_stage(scratch[4:]),
    )
    for k, out in enumerate((o0, o1, o2)):
        for r in range(3):
            out[pl.ds(r * (rows // 8), rows // 8), :] = compact(acc, k, r, rows)


def rest_kernel(
    slots, bits, odd, own, partner, feat_f, feat_g, own_1, partner_1, own_2, partner_2, own_out, partner_out, *scratch
):
    table, sems, acc = scratch[:3]
    rows = 8 * ((own.shape[0] - TABLE) // 7)
    tiles = rows // 8
    copies = table_copies((own, partner), table, sems)
    sums = ((own_out, own_1, own_2), (partner_out, partner_1, partner_2))
    for out, first, second in sums:
        out[...] = first[...] + second[...]
    for copy in copies:
        copy.wait()
    lookup, near = near_plan(odd[0], table, slots, bits)

    @pl.when(near > HEAD)
    def _():
        acc[...] = jnp.zeros_like(acc)
        pair_loop(lookup, HEAD, near, feat_f, feat_g, acc, 0, rows // 8, by_stage(scratch[3:]))
        for k, (out, _, _) in enumerate(sums):
            for r in range(3):
                out[pl.ds(r * tiles, tiles), :] += compact(acc, k, r, rows)


def call(function, ins, out_shape, scratch, smem_in=1, any_in=0):
    smem = pl.BlockSpec(memory_space=pltpu.SMEM)
    vmem = pl.BlockSpec(memory_space=pltpu.VMEM)
    anywhere = pl.BlockSpec(memory_space=pltpu.HBM)
    return pl.pallas_call(
        function,
        out_shape=out_shape,
        in_specs=[smem] * smem_in + [anywhere] * any_in + [vmem] * (len(ins) - smem_in - any_in),
        out_specs=[vmem] * len(out_shape),
        scratch_shapes=scratch,
        compiler_params=pltpu.CompilerParams(vmem_limit_bytes=40 * 2**20),
        cost_estimate=pl.CostEstimate(
            flops=30 * 10**9, bytes_accessed=4 * 10**6, transcendentals=0
        ),
    )(*ins)


def body(positions, normals, areas, pair_first, pair_second, pair_count):
    faces = areas.shape[0]
    clusters = faces // C
    bits = (clusters - 1).bit_length()
    tiles = faces // 128
    rows = 8 * tiles
    slots = pair_first.shape[0]
    devices = lax.axis_size(AXES)
    me = lax.axis_index(AXES)
    odd = jnp.reshape(me % 2, (1,))

    field = pair_second // clusters - me + 2
    code = (field << (2 * bits)) + ((pair_second % clusters) << bits) + pair_first % clusters
    unit = float(1 << (2 * bits))
    live = jnp.arange(slots, dtype=jnp.int32) < pair_count[0]
    code = jnp.where(live, code.astype(F32), 5.0 * unit).reshape(1, slots)
    (table,) = call(
        functools.partial(sort_kernel, unit),
        (code,),
        [jax.ShapeDtypeStruct((TABLE, 128), F32)],
        [],
        0,
    )
    geometry = jnp.concatenate([positions, normals, areas[None, :]], axis=0)
    geometry = geometry.reshape(7, tiles, 128).transpose(1, 0, 2).reshape(7 * tiles, 128)
    block = jnp.concatenate([geometry, table], axis=0)

    def permute(x, to):
        pairs = [(i, to(i)) for i in range(devices) if 0 <= to(i) < devices]
        return lax.ppermute(x, AXES, pairs)

    back = permute(block, lambda i: i + 2)
    partner = permute(block, lambda i: i ^ 1)
    part = jax.ShapeDtypeStruct((3 * tiles, 128), F32)
    f_rows = jax.ShapeDtypeStruct((6 * rows, 128), F32)
    g_rows = jax.ShapeDtypeStruct((4 * rows, 128), F32)

    def tables(count):
        return [pltpu.SMEM((count * TABLE, 128), F32), pltpu.SemaphoreType.DMA((count,))]

    own_1, partner_1, feat_f, feat_g = call(
        functools.partial(near_kernel, slots, bits),
        (odd, block, partner),
        [part, part, f_rows, g_rows],
        tables(2) + scratch_of(rows, 2),
    )
    own_2, partner_2, back_2 = call(
        functools.partial(far_kernel, slots, bits),
        (odd, block, partner, back, feat_f),
        [part] * 3,
        tables(3) + [pltpu.VMEM((2 * rows, 128), F32)] + scratch_of(rows, 3),
    )
    ahead_sum = permute(back_2, lambda i: i - 2)
    own_sum, partner_sum = call(
        functools.partial(rest_kernel, slots, bits),
        (odd, block, partner, feat_f, feat_g, own_1, partner_1, own_2, partner_2),
        [part, part],
        tables(2) + scratch_of(rows, 2),
    )
    total = own_sum + permute(partner_sum, lambda i: i ^ 1) + ahead_sum
    return total.reshape(3, faces)


def solution(mesh):
    in_specs = (
        P(None, AXES),
        P(None, AXES),
        P(AXES),
        P(AXES),
        P(AXES),
        P(AXES),
    )
    return jax.shard_map(
        body, mesh=mesh, in_specs=in_specs, out_specs=P(None, AXES), check_vma=False
    )
```
